32 devices in a mesh: gx: 16 (over z, y, x), gy: 2 (over core).
Axes of the slice: x: 2, y: 2, z: 4, core: 2. Of those that a mesh axis runs over, the one named last changes fastest.
Arguments:
- vectors: bfloat16 [4096, 768], P(('gx', 'gy')), may hold values from -6 to 6
- list_ids: int32 [4096], P(('gx', 'gy')), may hold values from 0 to 4095, as said below
- old_order: int32 [4096], replicated, may hold values from 0 to 4095, each once
- new_order: int32 [4096], replicated, may hold values from 0 to 4095, as said below
- centroids: bfloat16 [4096, 768], P('gx', 'gy'), may hold values from -6 to 6
- rotation: bfloat16 [768, 768], replicated, may hold values from -0.21875 to 0.21875
- codebook: bfloat16 [96, 8, 256], P('gy'), may hold values from -8 to 8
Outputs:
- quant_error: float32 [4096, 96], P(('gx', 'gy'))
- list_error: float32 [4096, 96], P('gx', 'gy')
The draws below stay inside these ranges and needn't reach their ends.
Inputs may be any that keep to these rules, and one draw needn't show every extreme that they name: `list_ids`: owner o holds the lists new_order[o * 256] to new_order[(o + 1) * 256 - 1]. Of the 128 vectors of one device, at most 20 name lists of one owner; in every draw some owner receives exactly 20 vectors from every device that shares its index of gy, and every device sends exactly 20 to some owner. `new_order`: each list once. `old_order`: each list once.
All inputs are finite; a program needn't handle non-finite values.
Results may differ from the reference program's by a relative error of at most 0.012.
Values may be sent and summed in bfloat16 or wider, within the bound.
No kernel may reach another device: no remote copies, remote signals or barrier semaphores. Data moves between devices by JAX's collectives and lax.ppermute only.
A program may use at most 128 MiB of HBM per device.

```python
import jax
import jax.numpy as jnp
from jax import lax

D = 768
NLIST = 4096
M = 96
K = 256
ROWS_DEV = 128
DS = 8
LIST_OWN = 256
CAP = 20
TOKENS = 4096


def plan_slots(key):
    return jax.random.permutation(jax.random.fold_in(key, 101), NLIST).astype(jnp.int32)


def draw_new_order(key, part):
    return plan_slots(key)


def draw_list_ids(key, part):
    list_order = plan_slots(key)
    base_key = jax.random.fold_in(key, 202)
    owners = NLIST // LIST_OWN
    devices = TOKENS // ROWS_DEV
    hot_owner = jax.random.randint(jax.random.fold_in(base_key, 1), (), 0, owners)
    floor_cap = ROWS_DEV // owners + 1
    slot_owner = jnp.repeat(jnp.arange(owners, dtype=jnp.int32), CAP)
    slot_pos = jnp.tile(jnp.arange(CAP, dtype=jnp.int32), owners)

    def one_device(device):
        device_key = jax.random.fold_in(base_key, device + 7)
        key_own = jax.random.fold_in(device_key, 1)
        key_caps = jax.random.fold_in(device_key, 2)
        key_rank = jax.random.fold_in(device_key, 3)
        key_shuffle = jax.random.fold_in(device_key, 4)
        key_within = jax.random.fold_in(device_key, 5)
        own_hot = (hot_owner + 1 + jax.random.randint(key_own, (), 0, owners - 1)) % owners
        owner_caps = jax.random.randint(key_caps, (owners,), floor_cap, CAP + 1)
        owner_range = jnp.arange(owners, dtype=jnp.int32)
        is_hot = (owner_range == hot_owner) | (owner_range == own_hot)
        owner_caps = jnp.where(is_hot, CAP, owner_caps)
        is_valid = slot_pos < owner_caps[slot_owner]
        forced = is_valid & ((slot_owner == hot_owner) | (slot_owner == own_hot))
        total_slots = owners * CAP
        ranking = jax.random.permutation(key_rank, total_slots).astype(jnp.int32)
        sort_key = jnp.where(forced, ranking, jnp.where(is_valid, ranking + total_slots, ranking + 2 * total_slots))
        chosen = jnp.argsort(sort_key, stable=True)[:ROWS_DEV]
        row_owner = jax.random.permutation(key_shuffle, slot_owner[chosen])
        within = jax.random.randint(key_within, (ROWS_DEV,), 0, LIST_OWN)
        return list_order[row_owner * LIST_OWN + within]
    return jax.vmap(one_device)(jnp.arange(devices, dtype=jnp.int32)).reshape(-1).astype(jnp.int32)


def block_scale(own_key, dims, pieces, low, largest):
    factor_of, own = 1.0, jax.random.fold_in(own_key, 6)
    for axis_at, parts in pieces:
        draws = jnp.exp(jax.random.uniform(jax.random.fold_in(own, axis_at), (parts,), jnp.float32, low / len(pieces), largest / len(pieces)))
        factor_of = factor_of * jnp.repeat(draws, dims[axis_at] // parts).reshape([-1 if axis == axis_at else 1 for axis in range(len(dims))])
    return factor_of


def bell_draw(rng, shape, deviation, reach, pieces=(), kind=jnp.bfloat16):
    result = deviation * jax.random.normal(rng, shape, jnp.float32)
    if pieces:
        result = result * block_scale(rng, shape, pieces, -0.22, 0.18)
    return jnp.clip(result, -reach, reach).astype(kind)


def setup_inputs(seed: int = 0) -> dict:
    arg_keys = jax.random.split(jax.random.key(seed), 8)
    return {
        "vectors": bell_draw(arg_keys[0], (TOKENS, D), 1.0, 6.0, ((0, 32),)),
        "list_ids": draw_list_ids(jax.random.fold_in(arg_keys[7], 71), 0),
        "old_order": jax.random.permutation(arg_keys[2], NLIST).astype(jnp.int32),
        "new_order": draw_new_order(jax.random.fold_in(arg_keys[7], 71), 0),
        "centroids": bell_draw(arg_keys[4], (NLIST, D), 1.0, 6.0, ((0, 16), (1, 2))),
        "rotation": bell_draw(arg_keys[5], (D, D), D ** -0.5, 0.21875),
        "codebook": bell_draw(arg_keys[6], (M, DS, K), 1.4, 8.0, ((0, 2),)),
    }


def subspace_errors(turned, codewords, code_norm):
    row_count = turned.shape[0]
    subspaces, sub_width, code_count = codewords.shape
    group_size = 8
    group_count = subspaces // group_size
    lowered = turned.astype(jnp.bfloat16).reshape(row_count, group_count, group_size, sub_width)
    lowered = jnp.moveaxis(lowered, 1, 0)
    squares = jnp.sum((turned * turned).reshape(row_count, group_count, group_size, sub_width), axis=3)
    squares = jnp.moveaxis(squares, 1, 0)
    book_groups = codewords.reshape(group_count, group_size, sub_width, code_count)
    norm_groups = code_norm.reshape(group_count, group_size, code_count)

    def one_group(operands):
        lowered_part, square_part, book_part, norm_part = operands
        inner_terms = jnp.einsum("rgd,gdk->rgk", lowered_part.astype(jnp.float32), book_part.astype(jnp.float32), precision=lax.Precision.HIGHEST)
        inner_terms = lax.optimization_barrier(inner_terms.astype(jnp.bfloat16)).astype(jnp.float32)
        distance = square_part[:, :, None] - 2.0 * inner_terms + norm_part[None, :, :]
        return jnp.min(distance, axis=2)

    nearest = lax.map(one_group, (lowered, squares, book_groups, norm_groups))
    return jnp.moveaxis(nearest, 0, 1).reshape(row_count, subspaces)


def reference(vectors, list_ids, old_order, new_order, centroids, rotation, codebook):
    list_total = old_order.shape[0]
    slot_index = jnp.arange(list_total, dtype=jnp.int32)
    where_old = jnp.zeros((list_total,), jnp.int32).at[old_order].set(slot_index)
    list_centroid = centroids[where_old]
    rot_cent = jnp.dot(list_centroid, rotation, preferred_element_type=jnp.float32)
    code_float = codebook.astype(jnp.float32)
    code_norm = jnp.sum(code_float * code_float, axis=1)
    block_count = vectors.shape[0] // ROWS_DEV

    def one_block(operands):
        block_rows, block_labels = operands
        turned = jnp.dot(block_rows, rotation, preferred_element_type=jnp.float32) - rot_cent[block_labels]
        return subspace_errors(turned, codebook, code_norm)

    quant_error = lax.map(one_block, (vectors.reshape(block_count, ROWS_DEV, D), list_ids.reshape(block_count, ROWS_DEV)))
    quant_error = quant_error.reshape(-1, M)
    list_sums = jax.ops.segment_sum(quant_error, list_ids, num_segments=list_total)
    counts = jax.ops.segment_sum(jnp.ones(list_ids.shape, jnp.float32), list_ids, num_segments=list_total)
    average = list_sums / jnp.maximum(counts, 1.0)[:, None]
    return quant_error, average[new_order]
```

```python
import functools

import jax
import jax.numpy as jnp
from jax import lax
from jax.experimental import pallas as pl
from jax.experimental.pallas import tpu as pltpu
from jax.sharding import PartitionSpec as P

LANES = 128
WIDE = 2 * LANES
F32 = jnp.float32
BF16 = jnp.bfloat16


def iota_f32(shape, axis):
    return lax.broadcasted_iota(jnp.int32, shape, axis).astype(F32)


def dot(a, b, contract=((1,), (0,))):
    return lax.dot_general(a, b, (contract, ((), ())), preferred_element_type=F32)


def slot_digits(ids_across, order_ref):
    found = jnp.zeros((LANES, LANES), F32)
    for block in range(order_ref.shape[0]):
        found = jnp.where(ids_across == order_ref[block : block + 1, :], float(block + 1), found)
    hit = (found > 0.0).astype(F32)
    block_of = (found - hit).astype(BF16)
    ones = jnp.ones((8, LANES), BF16)
    lanes = iota_f32((8, LANES), 1).astype(BF16)
    slot = dot(ones, block_of, ((1,), (1,))) * float(LANES) + dot(lanes, hit.astype(BF16), ((1,), (1,)))
    high = jnp.floor(slot * (1.0 / WIDE))
    return high, slot - high * WIDE


def prepare_kernel(own, ids_ref, old_ref, new_ref, vec_ref, rot_ref, book_ref, turned_ref, digit_ref, code_ref):
    ids_across = jnp.broadcast_to(ids_ref[...], (LANES, LANES)).astype(F32).T.astype(jnp.int32)
    old_high, old_low = slot_digits(ids_across, old_ref)
    new_high, new_low = slot_digits(ids_across, new_ref)
    row = lax.broadcasted_iota(jnp.int32, (8, LANES), 0)
    digits = jnp.where(row == 0, old_high, jnp.where(row == 1, old_low, jnp.where(row == 2, new_high, new_low)))
    digit_ref[...] = digits.astype(BF16)
    turned_ref[...] = dot(vec_ref[...], rot_ref[...]).T.astype(BF16)
    codes = book_ref.shape[2]
    first = lax.axis_index("gx") * own
    row = lax.broadcasted_iota(jnp.int32, (8, codes), 0)
    parts, tails = [], []
    for m in range(own):
        words = book_ref[first + m].astype(F32)
        zero = jnp.zeros_like(words)
        parts.append(jnp.concatenate([-2.0 * words if n == m else zero for n in range(own)], axis=1))
        norm = jnp.sum(words * words, axis=0, keepdims=True)
        top = norm.astype(BF16).astype(F32)
        middle = (norm - top).astype(BF16).astype(F32)
        low = norm - top - middle
        tails.append(jnp.where(row == 0, top, jnp.where(row == 1, middle, jnp.where(row == 2, low, 0.0))))
    parts.append(jnp.concatenate(tails, axis=1))
    code_ref[...] = jnp.concatenate(parts, axis=0).T.astype(BF16)


def pack_kernel(width, cent_ref, other_ref, rot_ref, turned_ref, digit_ref, out_ref):
    side = lax.axis_index("gy")
    half = cent_ref.shape[1]
    mine = cent_ref[pl.ds(side * LANES, LANES), :]
    other = other_ref[pl.ds(side * LANES, LANES), :]
    rotated = dot(mine, rot_ref[pl.ds(side * half, half), :])
    rotated += dot(other, rot_ref[pl.ds((1 - side) * half, half), :])
    cents = rotated.T
    vectors = turned_ref[...].astype(F32)
    digits = digit_ref[...].astype(F32)
    for device in range(out_ref.shape[0]):
        at = (device % 2) * half + (device // 2) * width
        block = jnp.concatenate([vectors[at : at + width], cents[at : at + width], digits], axis=0)
        out_ref[device] = block.astype(BF16)


def encode_kernel(own, sub_width, in_ref, code_ref, out_ref, table_ref, low_ref, square_ref):
    devices = in_ref.shape[0]
    tiles = devices // 2
    width = own * sub_width
    codes = code_ref.shape[0] // own

    def pair(tile, lo, hi):
        return jnp.concatenate([in_ref[2 * tile, lo:hi, :], in_ref[2 * tile + 1, lo:hi, :]], axis=1).astype(F32)

    digits = [pair(tile, 2 * width, 2 * width + 8) for tile in range(tiles)]
    for tile in range(tiles):
        table_ref[tile * width : (tile + 1) * width, :] = pair(tile, width, 2 * width)
    table = table_ref[...].astype(BF16)
    sub = iota_f32((WIDE, WIDE), 0)
    tail_row = lax.broadcasted_iota(jnp.int32, (8, WIDE), 0)
    tail = (tail_row < 3).astype(F32)
    for tile in range(tiles):
        hot = (sub == digits[tile][1:2]).astype(F32).astype(BF16)
        looked = dot(table, hot)
        high = jnp.broadcast_to(digits[tile][0:1], (width, WIDE))
        cent = jnp.zeros((width, WIDE), F32)
        for group in range(tiles):
            cent = jnp.where(high == float(group), looked[group * width : (group + 1) * width], cent)
        turned = pair(tile, 0, width) - cent
        lanes = slice(tile * WIDE, (tile + 1) * WIDE)
        low_ref[:, lanes] = jnp.concatenate([turned, tail], axis=0).astype(BF16)
        squared = turned * turned
        for m in range(own):
            square_ref[m : m + 1, lanes] = jnp.sum(
                squared[m * sub_width : (m + 1) * sub_width], axis=0, keepdims=True
            )
    code = code_ref[...]
    sums = jnp.zeros((tiles * 8, WIDE), F32)
    errors = []
    for tile in range(tiles):
        lanes = slice(tile * WIDE, (tile + 1) * WIDE)
        distance = dot(code, low_ref[:, lanes])
        nearest = jnp.concatenate(
            [jnp.min(distance[m * codes : (m + 1) * codes], axis=0, keepdims=True) for m in range(own)], axis=0
        )
        error = nearest + square_ref[0:own, lanes]
        errors.append(error)
        top = error.astype(BF16).astype(F32)
        rest = error - top
        pad = jnp.zeros((8 - 2 * own - 1, WIDE), F32)
        group_rows = jnp.concatenate([top, rest, jnp.ones((1, WIDE), F32), pad], axis=0)
        high = jnp.broadcast_to(digits[tile][2:3], (8, WIDE))
        spread = jnp.concatenate(
            [jnp.where(high == float(group), group_rows, 0.0) for group in range(tiles)], axis=0
        ).astype(BF16)
        hot = (sub == digits[tile][3:4]).astype(F32).astype(BF16)
        sums = sums + dot(spread, hot, ((1,), (1,)))
    for tile in range(tiles):
        group = sums[tile * 8 : (tile + 1) * 8]
        total = group[0:own] + group[own : 2 * own]
        mean = total / jnp.maximum(group[2 * own : 2 * own + 1], 1.0)
        pad = jnp.zeros((out_ref.shape[1] - 3 * own, LANES), F32)
        for side in range(2):
            block = jnp.concatenate(
                [errors[tile][:, side * LANES : (side + 1) * LANES], mean[:, :LANES], mean[:, LANES:], pad], axis=0
            )
            out_ref[2 * tile + side] = block.astype(BF16)


def finish_kernel(own, in_ref, quant_ref, list_ref, quant_rows, list_rows):
    tiles = in_ref.shape[0] // 2
    side = lax.axis_index("gy")
    for device in range(2 * tiles):
        at = ((device % 2) * tiles + device // 2) * own
        quant_rows[at : at + own, :] = in_ref[device].astype(F32)[0:own]
    for tile in range(tiles):
        block = in_ref[2 * tile + side].astype(F32)
        list_rows[tile * own : (tile + 1) * own, 0:LANES] = block[own : 2 * own]
        list_rows[tile * own : (tile + 1) * own, LANES:WIDE] = block[2 * own : 3 * own]
    quant_ref[...] = quant_rows[...].T
    list_ref[...] = list_rows[...].T


def on_device_by_column(vectors, list_ids, old_order, new_order, centroids, rotation, codebook):
    owners, sides = lax.axis_size("gx"), lax.axis_size("gy")
    devices = owners * sides
    subspaces, sub_width, codes = codebook.shape
    own = subspaces // owners
    width = own * sub_width
    features = vectors.shape[1]
    total = subspaces * sides
    other = lax.ppermute(centroids, "gy", [(0, 1), (1, 0)])
    turned, digits, code = pl.pallas_call(
        functools.partial(prepare_kernel, own),
        out_shape=(
            jax.ShapeDtypeStruct((features, LANES), BF16),
            jax.ShapeDtypeStruct((8, LANES), BF16),
            jax.ShapeDtypeStruct((own * codes, width + 8), BF16),
        ),
        name="prepare",
    )(
        list_ids.reshape(1, LANES),
        old_order.reshape(-1, LANES),
        new_order.reshape(-1, LANES),
        vectors,
        rotation,
        codebook,
    )
    outgoing = pl.pallas_call(
        functools.partial(pack_kernel, width),
        out_shape=jax.ShapeDtypeStruct((devices, 2 * width + 8, LANES), BF16),
        name="pack",
    )(centroids, other, rotation, turned, digits)
    incoming = lax.all_to_all(outgoing, ("gx", "gy"), split_axis=0, concat_axis=0, tiled=True)
    returning = pl.pallas_call(
        functools.partial(encode_kernel, own, sub_width),
        out_shape=jax.ShapeDtypeStruct((devices, 16, LANES), BF16),
        scratch_shapes=[
            pltpu.VMEM((owners * width, WIDE), F32),
            pltpu.VMEM((width + 8, devices * LANES), BF16),
            pltpu.VMEM((8, devices * LANES), F32),
        ],
        name="encode",
    )(incoming, code)
    returned = lax.all_to_all(returning, ("gx", "gy"), split_axis=0, concat_axis=0, tiled=True)
    return pl.pallas_call(
        functools.partial(finish_kernel, own),
        out_shape=(
            jax.ShapeDtypeStruct((LANES, total), F32),
            jax.ShapeDtypeStruct((WIDE, subspaces), F32),
        ),
        scratch_shapes=[pltpu.VMEM((total, LANES), F32), pltpu.VMEM((subspaces, WIDE), F32)],
        name="finish",
    )(returned)


def on_device(vectors, list_ids, old_order, new_order, centroids, rotation, codebook):
    owners, sides = lax.axis_size("gx"), lax.axis_size("gy")
    subspaces, sub_width, codes = codebook.shape
    own = subspaces // owners
    by_column = (
        sides == 2
        and own * owners == subspaces
        and 1 <= own <= 3
        and sub_width == 8
        and codes % LANES == 0
        and vectors.shape[0] == LANES
        and centroids.shape[0] == WIDE
        and old_order.shape[0] == owners * WIDE
        and owners <= WIDE
    )
    plan = on_device_by_column if by_column else on_device_by_owner
    return plan(vectors, list_ids, old_order, new_order, centroids, rotation, codebook)


def subspace_errors(turned, codewords, code_norm):
    row_count = turned.shape[0]
    subspaces, sub_width, code_count = codewords.shape
    group_size = 8
    group_count = subspaces // group_size
    lowered = turned.astype(jnp.bfloat16).reshape(row_count, group_count, group_size, sub_width)
    lowered = jnp.moveaxis(lowered, 1, 0)
    squares = jnp.sum(
        (turned * turned).reshape(row_count, group_count, group_size, sub_width), axis=3
    )
    squares = jnp.moveaxis(squares, 1, 0)
    book_groups = codewords.reshape(group_count, group_size, sub_width, code_count)
    norm_groups = code_norm.reshape(group_count, group_size, code_count)

    def one_group(operands):
        lowered_part, square_part, book_part, norm_part = operands
        inner_terms = jnp.einsum(
            "rgd,gdk->rgk", lowered_part, book_part, preferred_element_type=jnp.float32
        )
        inner_terms = lax.optimization_barrier(inner_terms.astype(jnp.bfloat16)).astype(jnp.float32)
        distance = square_part[:, :, None] - 2.0 * inner_terms + norm_part[None, :, :]
        return jnp.min(distance, axis=2)

    nearest = lax.map(one_group, (lowered, squares, book_groups, norm_groups))
    return jnp.moveaxis(nearest, 0, 1).reshape(row_count, subspaces)


def on_device_by_owner(vectors, list_ids, old_order, new_order, centroids, rotation, codebook):
    owners = lax.axis_size("gx")
    owner_index = lax.axis_index("gx")
    lists_own = centroids.shape[0]
    list_total = old_order.shape[0]
    rows_dev = vectors.shape[0]
    feature_width = vectors.shape[1]
    capacity = 5 * rows_dev // (2 * owners)
    own_lists = lax.dynamic_slice_in_dim(new_order, owner_index * lists_own, lists_own)
    select = (own_lists[:, None] == old_order[None, :]).astype(jnp.bfloat16)
    own_part = jnp.dot(
        select,
        lax.all_gather(centroids, "gx", axis=0, tiled=True),
        preferred_element_type=jnp.float32,
    )
    own_centroids = lax.all_gather(own_part.astype(jnp.bfloat16), "gy", axis=1, tiled=True)
    rot_cent = jnp.dot(own_centroids, rotation, preferred_element_type=jnp.float32)
    padded_cent = jnp.concatenate([rot_cent, jnp.zeros((1, feature_width), jnp.float32)], axis=0)
    codewords = lax.all_gather(codebook, "gy", axis=0, tiled=True)
    code_float = codewords.astype(jnp.float32)
    code_norm = jnp.sum(code_float * code_float, axis=1)
    subspaces = codewords.shape[0]
    slot_of = (
        jnp.zeros((list_total,), jnp.int32)
        .at[new_order]
        .set(jnp.arange(list_total, dtype=jnp.int32))
    )
    new_slot = slot_of[list_ids]
    dest_owner = new_slot // lists_own
    local_list = new_slot % lists_own
    owner_hits = (dest_owner[:, None] == jnp.arange(owners, dtype=jnp.int32)[None, :]).astype(
        jnp.int32
    )
    before = jnp.cumsum(owner_hits, axis=0) - owner_hits
    position = jnp.sum(before * owner_hits, axis=1)
    target = dest_owner * capacity + position
    labels_flat = jnp.full((owners * capacity,), lists_own, jnp.int32).at[target].set(local_list)
    outgoing = jnp.zeros((owners * capacity, feature_width), jnp.bfloat16).at[target].set(vectors)
    incoming = lax.all_to_all(
        outgoing.reshape(owners, capacity, feature_width),
        "gx",
        split_axis=0,
        concat_axis=0,
        tiled=True,
    )
    labels = lax.all_to_all(
        labels_flat.astype(jnp.bfloat16).reshape(owners, capacity),
        "gx",
        split_axis=0,
        concat_axis=0,
        tiled=True,
    )
    turned = jnp.dot(
        incoming.reshape(-1, feature_width), rotation, preferred_element_type=jnp.float32
    )
    finish_turned = turned
    label_rows = labels.reshape(-1).astype(jnp.int32)
    finish_turned = finish_turned - jnp.take(padded_cent, label_rows, axis=0)
    errors = subspace_errors(finish_turned, codewords, code_norm)
    results = errors.reshape(labels.shape[0], labels.shape[1], subspaces)
    returned = lax.all_to_all(results, "gx", split_axis=0, concat_axis=0, tiled=True)
    quant_error = returned.reshape(owners * capacity, subspaces)[target]
    label_rows = labels.reshape(-1).astype(jnp.int32)
    member = (label_rows[:, None] == jnp.arange(lists_own, dtype=jnp.int32)[None, :]).astype(
        jnp.float32
    )
    list_sums = jnp.einsum(
        "rl,rm->lm", member, results.reshape(-1, subspaces), precision=lax.Precision.HIGHEST
    )
    counts = jnp.sum(member, axis=0)
    list_sums, counts = lax.psum((list_sums, counts), "gy")
    average = list_sums / jnp.maximum(counts, 1.0)[:, None]
    own_columns = subspaces // lax.axis_size("gy")
    list_error = lax.dynamic_slice_in_dim(
        average, lax.axis_index("gy") * own_columns, own_columns, 1
    )
    return (quant_error, list_error)


def solution(mesh):
    in_specs = (
        P(("gx", "gy"), None),
        P(("gx", "gy")),
        P(),
        P(),
        P("gx", "gy"),
        P(),
        P("gy", None, None),
    )
    out_specs = (P(("gx", "gy"), None), P("gx", "gy"))
    return jax.shard_map(
        on_device, mesh=mesh, in_specs=in_specs, out_specs=out_specs, check_vma=False
    )
```

```python
import functools

import jax
import jax.numpy as jnp
from jax import lax
from jax.experimental import pallas as pl
from jax.experimental.pallas import tpu as pltpu
from jax.sharding import PartitionSpec as P

LANES = 128
WIDE = 2 * LANES
F32 = jnp.float32
BF16 = jnp.bfloat16


VMEM = pl.BlockSpec(memory_space=pltpu.VMEM)


def iota_f32(shape, axis):
    return lax.broadcasted_iota(jnp.int32, shape, axis).astype(F32)


def dot(a, b, contract=((1,), (0,))):
    return lax.dot_general(a, b, (contract, ((), ())), preferred_element_type=F32)


def slot_digits(ids_across, order_ref):
    found = jnp.zeros((LANES, LANES), F32)
    for block in range(order_ref.shape[0]):
        found = jnp.where(ids_across == order_ref[block : block + 1, :], float(block + 1), found)
    hit = (found > 0.0).astype(F32)
    block_of = (found - hit).astype(BF16)
    ones = jnp.ones((8, LANES), BF16)
    lanes = iota_f32((8, LANES), 1).astype(BF16)
    slot = dot(ones, block_of, ((1,), (1,))) * float(LANES) + dot(lanes, hit.astype(BF16), ((1,), (1,)))
    high = jnp.floor(slot * (1.0 / WIDE))
    return high, slot - high * WIDE


def prepare_kernel(own, ids_ref, old_ref, new_ref, vec_ref, rot_ref, book_ref, turned_ref, digit_ref, code_ref):
    ids_across = jnp.broadcast_to(ids_ref[...], (LANES, LANES)).astype(F32).T.astype(jnp.int32)
    old_high, old_low = slot_digits(ids_across, old_ref)
    new_high, new_low = slot_digits(ids_across, new_ref)
    row = lax.broadcasted_iota(jnp.int32, (8, LANES), 0)
    digits = jnp.where(row == 0, old_high, jnp.where(row == 1, old_low, jnp.where(row == 2, new_high, new_low)))
    digit_ref[...] = digits.astype(BF16)
    turned_ref[...] = dot(vec_ref[...], rot_ref[...]).T.astype(BF16)
    codes = book_ref.shape[2]
    first = lax.axis_index("gx") * own
    row = lax.broadcasted_iota(jnp.int32, (8, codes), 0)
    parts, tails = [], []
    for m in range(own):
        words = book_ref[first + m].astype(F32)
        zero = jnp.zeros_like(words)
        parts.append(jnp.concatenate([-2.0 * words if n == m else zero for n in range(own)], axis=1))
        norm = jnp.sum(words * words, axis=0, keepdims=True)
        top = norm.astype(BF16).astype(F32)
        middle = (norm - top).astype(BF16).astype(F32)
        low = norm - top - middle
        tails.append(jnp.where(row == 0, top, jnp.where(row == 1, middle, jnp.where(row == 2, low, 0.0))))
    parts.append(jnp.concatenate(tails, axis=1))
    code_ref[...] = jnp.concatenate(parts, axis=0).T.astype(BF16)


def pack_kernel(width, cent_ref, other_ref, rot_ref, turned_ref, digit_ref, out_ref):
    side = lax.axis_index("gy")
    half = cent_ref.shape[1]
    mine = cent_ref[pl.ds(side * LANES, LANES), :]
    other = other_ref[pl.ds(side * LANES, LANES), :]
    rotated = dot(mine, rot_ref[pl.ds(side * half, half), :])
    rotated += dot(other, rot_ref[pl.ds((1 - side) * half, half), :])
    cents = rotated.T
    vectors = turned_ref[...].astype(F32)
    digits = digit_ref[...].astype(F32)
    for device in range(out_ref.shape[0]):
        at = (device % 2) * half + (device // 2) * width
        block = jnp.concatenate([vectors[at : at + width], cents[at : at + width], digits], axis=0)
        out_ref[device] = block.astype(BF16)


def encode_kernel(own, sub_width, in_ref, code_ref, out_ref, table_ref, low_ref, square_ref):
    devices = in_ref.shape[0]
    tiles = devices // 2
    width = own * sub_width
    codes = code_ref.shape[0] // own

    def pair(tile, lo, hi):
        return jnp.concatenate([in_ref[2 * tile, lo:hi, :], in_ref[2 * tile + 1, lo:hi, :]], axis=1).astype(F32)

    digits = [pair(tile, 2 * width, 2 * width + 8) for tile in range(tiles)]
    for tile in range(tiles):
        table_ref[tile * width : (tile + 1) * width, :] = pair(tile, width, 2 * width)
    table = table_ref[...].astype(BF16)
    sub = iota_f32((WIDE, WIDE), 0)
    tail_row = lax.broadcasted_iota(jnp.int32, (8, WIDE), 0)
    tail = (tail_row < 3).astype(F32)
    for tile in range(tiles):
        hot = (sub == digits[tile][1:2]).astype(F32).astype(BF16)
        looked = dot(table, hot)
        high = jnp.broadcast_to(digits[tile][0:1], (width, WIDE))
        cent = jnp.zeros((width, WIDE), F32)
        for group in range(tiles):
            cent = jnp.where(high == float(group), looked[group * width : (group + 1) * width], cent)
        turned = pair(tile, 0, width) - cent
        lanes = slice(tile * WIDE, (tile + 1) * WIDE)
        low_ref[:, lanes] = jnp.concatenate([turned, tail], axis=0).astype(BF16)
        squared = turned * turned
        for m in range(own):
            square_ref[m : m + 1, lanes] = jnp.sum(
                squared[m * sub_width : (m + 1) * sub_width], axis=0, keepdims=True
            )
    code = code_ref[...]
    sums = jnp.zeros((tiles * 8, WIDE), F32)
    errors = []
    for tile in range(tiles):
        lanes = slice(tile * WIDE, (tile + 1) * WIDE)
        distance = dot(code, low_ref[:, lanes])
        nearest = jnp.concatenate(
            [jnp.min(distance[m * codes : (m + 1) * codes], axis=0, keepdims=True) for m in range(own)], axis=0
        )
        error = nearest + square_ref[0:own, lanes]
        errors.append(error)
        top = error.astype(BF16).astype(F32)
        rest = error - top
        pad = jnp.zeros((8 - 2 * own - 1, WIDE), F32)
        group_rows = jnp.concatenate([top, rest, jnp.ones((1, WIDE), F32), pad], axis=0)
        high = jnp.broadcast_to(digits[tile][2:3], (8, WIDE))
        spread = jnp.concatenate(
            [jnp.where(high == float(group), group_rows, 0.0) for group in range(tiles)], axis=0
        ).astype(BF16)
        hot = (sub == digits[tile][3:4]).astype(F32).astype(BF16)
        sums = sums + dot(spread, hot, ((1,), (1,)))
    for tile in range(tiles):
        group = sums[tile * 8 : (tile + 1) * 8]
        total = group[0:own] + group[own : 2 * own]
        mean = total / jnp.maximum(group[2 * own : 2 * own + 1], 1.0)
        pad = jnp.zeros((out_ref.shape[1] - 3 * own, LANES), F32)
        for side in range(2):
            block = jnp.concatenate(
                [errors[tile][:, side * LANES : (side + 1) * LANES], mean[:, :LANES], mean[:, LANES:], pad], axis=0
            )
            out_ref[2 * tile + side] = block.astype(BF16)


def finish_kernel(own, in_ref, quant_ref, list_ref):
    tiles = in_ref.shape[0] // 2
    side = lax.axis_index("gy")
    for device in range(2 * tiles):
        at = ((device % 2) * tiles + device // 2) * own
        quant_ref[at : at + own, :] = in_ref[device].astype(F32)[0:own]
    for tile in range(tiles):
        block = in_ref[2 * tile + side].astype(F32)
        list_ref[tile * own : (tile + 1) * own, 0:LANES] = block[own : 2 * own]
        list_ref[tile * own : (tile + 1) * own, LANES:WIDE] = block[2 * own : 3 * own]


def on_device_by_column(vectors, list_ids, old_order, new_order, centroids, rotation, codebook):
    owners, sides = lax.axis_size("gx"), lax.axis_size("gy")
    devices = owners * sides
    subspaces, sub_width, codes = codebook.shape
    own = subspaces // owners
    width = own * sub_width
    features = vectors.shape[1]
    total = subspaces * sides
    other = lax.ppermute(centroids, "gy", [(0, 1), (1, 0)])
    turned, digits, code = pl.pallas_call(
        functools.partial(prepare_kernel, own),
        out_shape=(
            jax.ShapeDtypeStruct((features, LANES), BF16),
            jax.ShapeDtypeStruct((8, LANES), BF16),
            jax.ShapeDtypeStruct((own * codes, width + 8), BF16),
        ),
        in_specs=[VMEM] * 6,
        out_specs=(VMEM, VMEM, VMEM),
        name="prepare",
    )(
        list_ids.reshape(1, LANES),
        old_order.reshape(-1, LANES),
        new_order.reshape(-1, LANES),
        vectors,
        rotation,
        codebook,
    )
    outgoing = pl.pallas_call(
        functools.partial(pack_kernel, width),
        out_shape=jax.ShapeDtypeStruct((devices, 2 * width + 8, LANES), BF16),
        in_specs=[VMEM] * 5,
        out_specs=VMEM,
        name="pack",
    )(centroids, other, rotation, turned, digits)
    incoming = lax.all_to_all(outgoing, ("gx", "gy"), split_axis=0, concat_axis=0, tiled=True)
    returning = pl.pallas_call(
        functools.partial(encode_kernel, own, sub_width),
        out_shape=jax.ShapeDtypeStruct((devices, 16, LANES), BF16),
        scratch_shapes=[
            pltpu.VMEM((owners * width, WIDE), F32),
            pltpu.VMEM((width + 8, devices * LANES), BF16),
            pltpu.VMEM((8, devices * LANES), F32),
        ],
        in_specs=[VMEM] * 2,
        out_specs=VMEM,
        name="encode",
    )(incoming, code)
    returned = lax.all_to_all(returning, ("gx", "gy"), split_axis=0, concat_axis=0, tiled=True)
    quant_error, list_error = pl.pallas_call(
        functools.partial(finish_kernel, own),
        out_shape=(
            jax.ShapeDtypeStruct((total, LANES), F32),
            jax.ShapeDtypeStruct((subspaces, WIDE), F32),
        ),
        in_specs=[VMEM],
        out_specs=(VMEM, VMEM),
        name="finish",
    )(returned)
    return quant_error.T, list_error.T


def on_device(vectors, list_ids, old_order, new_order, centroids, rotation, codebook):
    owners, sides = lax.axis_size("gx"), lax.axis_size("gy")
    subspaces, sub_width, codes = codebook.shape
    own = subspaces // owners
    by_column = (
        sides == 2
        and own * owners == subspaces
        and 1 <= own <= 3
        and sub_width == 8
        and codes % LANES == 0
        and vectors.shape[0] == LANES
        and centroids.shape[0] == WIDE
        and old_order.shape[0] == owners * WIDE
        and owners <= WIDE
    )
    plan = on_device_by_column if by_column else on_device_by_owner
    return plan(vectors, list_ids, old_order, new_order, centroids, rotation, codebook)


def subspace_errors(turned, codewords, code_norm):
    row_count = turned.shape[0]
    subspaces, sub_width, code_count = codewords.shape
    group_size = 8
    group_count = subspaces // group_size
    lowered = turned.astype(jnp.bfloat16).reshape(row_count, group_count, group_size, sub_width)
    lowered = jnp.moveaxis(lowered, 1, 0)
    squares = jnp.sum(
        (turned * turned).reshape(row_count, group_count, group_size, sub_width), axis=3
    )
    squares = jnp.moveaxis(squares, 1, 0)
    book_groups = codewords.reshape(group_count, group_size, sub_width, code_count)
    norm_groups = code_norm.reshape(group_count, group_size, code_count)

    def one_group(operands):
        lowered_part, square_part, book_part, norm_part = operands
        inner_terms = jnp.einsum(
            "rgd,gdk->rgk", lowered_part, book_part, preferred_element_type=jnp.float32
        )
        inner_terms = lax.optimization_barrier(inner_terms.astype(jnp.bfloat16)).astype(jnp.float32)
        distance = square_part[:, :, None] - 2.0 * inner_terms + norm_part[None, :, :]
        return jnp.min(distance, axis=2)

    nearest = lax.map(one_group, (lowered, squares, book_groups, norm_groups))
    return jnp.moveaxis(nearest, 0, 1).reshape(row_count, subspaces)


def on_device_by_owner(vectors, list_ids, old_order, new_order, centroids, rotation, codebook):
    owners = lax.axis_size("gx")
    owner_index = lax.axis_index("gx")
    lists_own = centroids.shape[0]
    list_total = old_order.shape[0]
    rows_dev = vectors.shape[0]
    feature_width = vectors.shape[1]
    capacity = 5 * rows_dev // (2 * owners)
    own_lists = lax.dynamic_slice_in_dim(new_order, owner_index * lists_own, lists_own)
    select = (own_lists[:, None] == old_order[None, :]).astype(jnp.bfloat16)
    own_part = jnp.dot(
        select,
        lax.all_gather(centroids, "gx", axis=0, tiled=True),
        preferred_element_type=jnp.float32,
    )
    own_centroids = lax.all_gather(own_part.astype(jnp.bfloat16), "gy", axis=1, tiled=True)
    rot_cent = jnp.dot(own_centroids, rotation, preferred_element_type=jnp.float32)
    padded_cent = jnp.concatenate([rot_cent, jnp.zeros((1, feature_width), jnp.float32)], axis=0)
    codewords = lax.all_gather(codebook, "gy", axis=0, tiled=True)
    code_float = codewords.astype(jnp.float32)
    code_norm = jnp.sum(code_float * code_float, axis=1)
    subspaces = codewords.shape[0]
    slot_of = (
        jnp.zeros((list_total,), jnp.int32)
        .at[new_order]
        .set(jnp.arange(list_total, dtype=jnp.int32))
    )
    new_slot = slot_of[list_ids]
    dest_owner = new_slot // lists_own
    local_list = new_slot % lists_own
    owner_hits = (dest_owner[:, None] == jnp.arange(owners, dtype=jnp.int32)[None, :]).astype(
        jnp.int32
    )
    before = jnp.cumsum(owner_hits, axis=0) - owner_hits
    position = jnp.sum(before * owner_hits, axis=1)
    target = dest_owner * capacity + position
    labels_flat = jnp.full((owners * capacity,), lists_own, jnp.int32).at[target].set(local_list)
    outgoing = jnp.zeros((owners * capacity, feature_width), jnp.bfloat16).at[target].set(vectors)
    incoming = lax.all_to_all(
        outgoing.reshape(owners, capacity, feature_width),
        "gx",
        split_axis=0,
        concat_axis=0,
        tiled=True,
    )
    labels = lax.all_to_all(
        labels_flat.astype(jnp.bfloat16).reshape(owners, capacity),
        "gx",
        split_axis=0,
        concat_axis=0,
        tiled=True,
    )
    turned = jnp.dot(
        incoming.reshape(-1, feature_width), rotation, preferred_element_type=jnp.float32
    )
    finish_turned = turned
    label_rows = labels.reshape(-1).astype(jnp.int32)
    finish_turned = finish_turned - jnp.take(padded_cent, label_rows, axis=0)
    errors = subspace_errors(finish_turned, codewords, code_norm)
    results = errors.reshape(labels.shape[0], labels.shape[1], subspaces)
    returned = lax.all_to_all(results, "gx", split_axis=0, concat_axis=0, tiled=True)
    quant_error = returned.reshape(owners * capacity, subspaces)[target]
    label_rows = labels.reshape(-1).astype(jnp.int32)
    member = (label_rows[:, None] == jnp.arange(lists_own, dtype=jnp.int32)[None, :]).astype(
        jnp.float32
    )
    list_sums = jnp.einsum(
        "rl,rm->lm", member, results.reshape(-1, subspaces), precision=lax.Precision.HIGHEST
    )
    counts = jnp.sum(member, axis=0)
    list_sums, counts = lax.psum((list_sums, counts), "gy")
    average = list_sums / jnp.maximum(counts, 1.0)[:, None]
    own_columns = subspaces // lax.axis_size("gy")
    list_error = lax.dynamic_slice_in_dim(
        average, lax.axis_index("gy") * own_columns, own_columns, 1
    )
    return (quant_error, list_error)


def solution(mesh):
    in_specs = (
        P(("gx", "gy"), None),
        P(("gx", "gy")),
        P(),
        P(),
        P("gx", "gy"),
        P(),
        P("gy", None, None),
    )
    out_specs = (P(("gx", "gy"), None), P("gx", "gy"))
    return jax.shard_map(
        on_device, mesh=mesh, in_specs=in_specs, out_specs=out_specs, check_vma=False
    )
```

```python
import functools

import jax
import jax.numpy as jnp
from jax import lax
from jax.experimental import pallas as pl
from jax.experimental.pallas import tpu as pltpu
from jax.sharding import PartitionSpec as P

LANES = 128
WIDE = 2 * LANES
F32 = jnp.float32
BF16 = jnp.bfloat16


VMEM = pl.BlockSpec(memory_space=pltpu.VMEM)


def on_chip(array):
    return pltpu.with_memory_space_constraint(array, pltpu.VMEM)


def iota_f32(shape, axis):
    return lax.broadcasted_iota(jnp.int32, shape, axis).astype(F32)


def dot(a, b, contract=((1,), (0,))):
    return lax.dot_general(a, b, (contract, ((), ())), preferred_element_type=F32)


def slot_digits(ids_across, order_ref):
    found = jnp.zeros((LANES, LANES), F32)
    for block in range(order_ref.shape[0]):
        found = jnp.where(ids_across == order_ref[block : block + 1, :], float(block + 1), found)
    hit = (found > 0.0).astype(F32)
    block_of = (found - hit).astype(BF16)
    ones = jnp.ones((8, LANES), BF16)
    lanes = iota_f32((8, LANES), 1).astype(BF16)
    slot = dot(ones, block_of, ((1,), (1,))) * float(LANES) + dot(lanes, hit.astype(BF16), ((1,), (1,)))
    high = jnp.floor(slot * (1.0 / WIDE))
    return high, slot - high * WIDE


def prepare_kernel(own, ids_ref, old_ref, new_ref, vec_ref, rot_ref, book_ref, turned_ref, digit_ref, code_ref):
    ids_across = jnp.broadcast_to(ids_ref[...], (LANES, LANES)).astype(F32).T.astype(jnp.int32)
    old_high, old_low = slot_digits(ids_across, old_ref)
    new_high, new_low = slot_digits(ids_across, new_ref)
    row = lax.broadcasted_iota(jnp.int32, (8, LANES), 0)
    digits = jnp.where(row == 0, old_high, jnp.where(row == 1, old_low, jnp.where(row == 2, new_high, new_low)))
    digit_ref[...] = digits.astype(BF16)
    turned_ref[...] = dot(vec_ref[...], rot_ref[...]).T.astype(BF16)
    codes = book_ref.shape[2]
    first = lax.axis_index("gx") * own
    row = lax.broadcasted_iota(jnp.int32, (8, codes), 0)
    parts, tails = [], []
    for m in range(own):
        words = book_ref[first + m].astype(F32)
        zero = jnp.zeros_like(words)
        parts.append(jnp.concatenate([-2.0 * words if n == m else zero for n in range(own)], axis=1))
        norm = jnp.sum(words * words, axis=0, keepdims=True)
        top = norm.astype(BF16).astype(F32)
        middle = (norm - top).astype(BF16).astype(F32)
        low = norm - top - middle
        tails.append(jnp.where(row == 0, top, jnp.where(row == 1, middle, jnp.where(row == 2, low, 0.0))))
    parts.append(jnp.concatenate(tails, axis=1))
    code_ref[...] = jnp.concatenate(parts, axis=0).T.astype(BF16)


def pack_kernel(width, cent_ref, other_ref, rot_ref, turned_ref, digit_ref, out_ref):
    side = lax.axis_index("gy")
    half = cent_ref.shape[1]
    mine = cent_ref[pl.ds(side * LANES, LANES), :]
    other = other_ref[pl.ds(side * LANES, LANES), :]
    rotated = dot(mine, rot_ref[pl.ds(side * half, half), :])
    rotated += dot(other, rot_ref[pl.ds((1 - side) * half, half), :])
    cents = rotated.T
    vectors = turned_ref[...].astype(F32)
    digits = digit_ref[...].astype(F32)
    for device in range(out_ref.shape[0]):
        at = (device % 2) * half + (device // 2) * width
        block = jnp.concatenate([vectors[at : at + width], cents[at : at + width], digits], axis=0)
        out_ref[device] = block.astype(BF16)


def encode_kernel(own, sub_width, in_ref, code_ref, out_ref, table_ref, low_ref, square_ref):
    devices = in_ref.shape[0]
    tiles = devices // 2
    width = own * sub_width
    codes = code_ref.shape[0] // own

    def pair(tile, lo, hi):
        return jnp.concatenate([in_ref[2 * tile, lo:hi, :], in_ref[2 * tile + 1, lo:hi, :]], axis=1).astype(F32)

    digits = [pair(tile, 2 * width, 2 * width + 8) for tile in range(tiles)]
    for tile in range(tiles):
        table_ref[tile * width : (tile + 1) * width, :] = pair(tile, width, 2 * width)
    table = table_ref[...].astype(BF16)
    sub = iota_f32((WIDE, WIDE), 0)
    tail_row = lax.broadcasted_iota(jnp.int32, (8, WIDE), 0)
    tail = (tail_row < 3).astype(F32)
    for tile in range(tiles):
        hot = (sub == digits[tile][1:2]).astype(F32).astype(BF16)
        looked = dot(table, hot)
        high = jnp.broadcast_to(digits[tile][0:1], (width, WIDE))
        cent = jnp.zeros((width, WIDE), F32)
        for group in range(tiles):
            cent = jnp.where(high == float(group), looked[group * width : (group + 1) * width], cent)
        turned = pair(tile, 0, width) - cent
        lanes = slice(tile * WIDE, (tile + 1) * WIDE)
        low_ref[:, lanes] = jnp.concatenate([turned, tail], axis=0).astype(BF16)
        squared = turned * turned
        for m in range(own):
            square_ref[m : m + 1, lanes] = jnp.sum(
                squared[m * sub_width : (m + 1) * sub_width], axis=0, keepdims=True
            )
    code = code_ref[...]
    sums = jnp.zeros((tiles * 8, WIDE), F32)
    errors = []
    for tile in range(tiles):
        lanes = slice(tile * WIDE, (tile + 1) * WIDE)
        distance = dot(code, low_ref[:, lanes])
        nearest = jnp.concatenate(
            [jnp.min(distance[m * codes : (m + 1) * codes], axis=0, keepdims=True) for m in range(own)], axis=0
        )
        error = nearest + square_ref[0:own, lanes]
        errors.append(error)
        top = error.astype(BF16).astype(F32)
        rest = error - top
        pad = jnp.zeros((8 - 2 * own - 1, WIDE), F32)
        group_rows = jnp.concatenate([top, rest, jnp.ones((1, WIDE), F32), pad], axis=0)
        high = jnp.broadcast_to(digits[tile][2:3], (8, WIDE))
        spread = jnp.concatenate(
            [jnp.where(high == float(group), group_rows, 0.0) for group in range(tiles)], axis=0
        ).astype(BF16)
        hot = (sub == digits[tile][3:4]).astype(F32).astype(BF16)
        sums = sums + dot(spread, hot, ((1,), (1,)))
    for tile in range(tiles):
        group = sums[tile * 8 : (tile + 1) * 8]
        total = group[0:own] + group[own : 2 * own]
        mean = total / jnp.maximum(group[2 * own : 2 * own + 1], 1.0)
        pad = jnp.zeros((out_ref.shape[1] - 3 * own, LANES), F32)
        for side in range(2):
            block = jnp.concatenate(
                [errors[tile][:, side * LANES : (side + 1) * LANES], mean[:, :LANES], mean[:, LANES:], pad], axis=0
            )
            out_ref[2 * tile + side] = block.astype(BF16)


def finish_kernel(own, in_ref, quant_ref, list_ref):
    tiles = in_ref.shape[0] // 2
    side = lax.axis_index("gy")
    for device in range(2 * tiles):
        at = ((device % 2) * tiles + device // 2) * own
        quant_ref[at : at + own, :] = in_ref[device].astype(F32)[0:own]
    for tile in range(tiles):
        block = in_ref[2 * tile + side].astype(F32)
        list_ref[tile * own : (tile + 1) * own, 0:LANES] = block[own : 2 * own]
        list_ref[tile * own : (tile + 1) * own, LANES:WIDE] = block[2 * own : 3 * own]


def on_device_by_column(vectors, list_ids, old_order, new_order, centroids, rotation, codebook):
    owners, sides = lax.axis_size("gx"), lax.axis_size("gy")
    devices = owners * sides
    subspaces, sub_width, codes = codebook.shape
    own = subspaces // owners
    width = own * sub_width
    features = vectors.shape[1]
    total = subspaces * sides
    other = on_chip(lax.ppermute(centroids, "gy", [(0, 1), (1, 0)]))
    rotation = on_chip(rotation)
    turned, digits, code = pl.pallas_call(
        functools.partial(prepare_kernel, own),
        out_shape=(
            pltpu.VMEM((features, LANES), BF16),
            pltpu.VMEM((8, LANES), BF16),
            pltpu.VMEM((own * codes, width + 8), BF16),
        ),
        in_specs=[VMEM] * 6,
        out_specs=(VMEM, VMEM, VMEM),
        name="prepare",
    )(
        list_ids.reshape(1, LANES),
        old_order.reshape(-1, LANES),
        new_order.reshape(-1, LANES),
        vectors,
        rotation,
        codebook,
    )
    outgoing = pl.pallas_call(
        functools.partial(pack_kernel, width),
        out_shape=pltpu.VMEM((devices, 2 * width + 8, LANES), BF16),
        in_specs=[VMEM] * 5,
        out_specs=VMEM,
        name="pack",
    )(on_chip(centroids), other, rotation, on_chip(turned), on_chip(digits))
    incoming = lax.all_to_all(outgoing, ("gx", "gy"), split_axis=0, concat_axis=0, tiled=True)
    returning = pl.pallas_call(
        functools.partial(encode_kernel, own, sub_width),
        out_shape=pltpu.VMEM((devices, 16, LANES), BF16),
        scratch_shapes=[
            pltpu.VMEM((owners * width, WIDE), F32),
            pltpu.VMEM((width + 8, devices * LANES), BF16),
            pltpu.VMEM((8, devices * LANES), F32),
        ],
        in_specs=[VMEM] * 2,
        out_specs=VMEM,
        name="encode",
    )(on_chip(incoming), on_chip(code))
    returned = lax.all_to_all(returning, ("gx", "gy"), split_axis=0, concat_axis=0, tiled=True)
    quant_error, list_error = pl.pallas_call(
        functools.partial(finish_kernel, own),
        out_shape=(
            jax.ShapeDtypeStruct((total, LANES), F32),
            jax.ShapeDtypeStruct((subspaces, WIDE), F32),
        ),
        in_specs=[VMEM],
        out_specs=(VMEM, VMEM),
        name="finish",
    )(on_chip(returned))
    return quant_error.T, list_error.T


def on_device(vectors, list_ids, old_order, new_order, centroids, rotation, codebook):
    owners, sides = lax.axis_size("gx"), lax.axis_size("gy")
    subspaces, sub_width, codes = codebook.shape
    own = subspaces // owners
    by_column = (
        sides == 2
        and own * owners == subspaces
        and 1 <= own <= 3
        and sub_width == 8
        and codes % LANES == 0
        and vectors.shape[0] == LANES
        and centroids.shape[0] == WIDE
        and old_order.shape[0] == owners * WIDE
        and owners <= WIDE
    )
    plan = on_device_by_column if by_column else on_device_by_owner
    return plan(vectors, list_ids, old_order, new_order, centroids, rotation, codebook)


def subspace_errors(turned, codewords, code_norm):
    row_count = turned.shape[0]
    subspaces, sub_width, code_count = codewords.shape
    group_size = 8
    group_count = subspaces // group_size
    lowered = turned.astype(jnp.bfloat16).reshape(row_count, group_count, group_size, sub_width)
    lowered = jnp.moveaxis(lowered, 1, 0)
    squares = jnp.sum(
        (turned * turned).reshape(row_count, group_count, group_size, sub_width), axis=3
    )
    squares = jnp.moveaxis(squares, 1, 0)
    book_groups = codewords.reshape(group_count, group_size, sub_width, code_count)
    norm_groups = code_norm.reshape(group_count, group_size, code_count)

    def one_group(operands):
        lowered_part, square_part, book_part, norm_part = operands
        inner_terms = jnp.einsum(
            "rgd,gdk->rgk", lowered_part, book_part, preferred_element_type=jnp.float32
        )
        inner_terms = lax.optimization_barrier(inner_terms.astype(jnp.bfloat16)).astype(jnp.float32)
        distance = square_part[:, :, None] - 2.0 * inner_terms + norm_part[None, :, :]
        return jnp.min(distance, axis=2)

    nearest = lax.map(one_group, (lowered, squares, book_groups, norm_groups))
    return jnp.moveaxis(nearest, 0, 1).reshape(row_count, subspaces)


def on_device_by_owner(vectors, list_ids, old_order, new_order, centroids, rotation, codebook):
    owners = lax.axis_size("gx")
    owner_index = lax.axis_index("gx")
    lists_own = centroids.shape[0]
    list_total = old_order.shape[0]
    rows_dev = vectors.shape[0]
    feature_width = vectors.shape[1]
    capacity = 5 * rows_dev // (2 * owners)
    own_lists = lax.dynamic_slice_in_dim(new_order, owner_index * lists_own, lists_own)
    select = (own_lists[:, None] == old_order[None, :]).astype(jnp.bfloat16)
    own_part = jnp.dot(
        select,
        lax.all_gather(centroids, "gx", axis=0, tiled=True),
        preferred_element_type=jnp.float32,
    )
    own_centroids = lax.all_gather(own_part.astype(jnp.bfloat16), "gy", axis=1, tiled=True)
    rot_cent = jnp.dot(own_centroids, rotation, preferred_element_type=jnp.float32)
    padded_cent = jnp.concatenate([rot_cent, jnp.zeros((1, feature_width), jnp.float32)], axis=0)
    codewords = lax.all_gather(codebook, "gy", axis=0, tiled=True)
    code_float = codewords.astype(jnp.float32)
    code_norm = jnp.sum(code_float * code_float, axis=1)
    subspaces = codewords.shape[0]
    slot_of = (
        jnp.zeros((list_total,), jnp.int32)
        .at[new_order]
        .set(jnp.arange(list_total, dtype=jnp.int32))
    )
    new_slot = slot_of[list_ids]
    dest_owner = new_slot // lists_own
    local_list = new_slot % lists_own
    owner_hits = (dest_owner[:, None] == jnp.arange(owners, dtype=jnp.int32)[None, :]).astype(
        jnp.int32
    )
    before = jnp.cumsum(owner_hits, axis=0) - owner_hits
    position = jnp.sum(before * owner_hits, axis=1)
    target = dest_owner * capacity + position
    labels_flat = jnp.full((owners * capacity,), lists_own, jnp.int32).at[target].set(local_list)
    outgoing = jnp.zeros((owners * capacity, feature_width), jnp.bfloat16).at[target].set(vectors)
    incoming = lax.all_to_all(
        outgoing.reshape(owners, capacity, feature_width),
        "gx",
        split_axis=0,
        concat_axis=0,
        tiled=True,
    )
    labels = lax.all_to_all(
        labels_flat.astype(jnp.bfloat16).reshape(owners, capacity),
        "gx",
        split_axis=0,
        concat_axis=0,
        tiled=True,
    )
    turned = jnp.dot(
        incoming.reshape(-1, feature_width), rotation, preferred_element_type=jnp.float32
    )
    finish_turned = turned
    label_rows = labels.reshape(-1).astype(jnp.int32)
    finish_turned = finish_turned - jnp.take(padded_cent, label_rows, axis=0)
    errors = subspace_errors(finish_turned, codewords, code_norm)
    results = errors.reshape(labels.shape[0], labels.shape[1], subspaces)
    returned = lax.all_to_all(results, "gx", split_axis=0, concat_axis=0, tiled=True)
    quant_error = returned.reshape(owners * capacity, subspaces)[target]
    label_rows = labels.reshape(-1).astype(jnp.int32)
    member = (label_rows[:, None] == jnp.arange(lists_own, dtype=jnp.int32)[None, :]).astype(
        jnp.float32
    )
    list_sums = jnp.einsum(
        "rl,rm->lm", member, results.reshape(-1, subspaces), precision=lax.Precision.HIGHEST
    )
    counts = jnp.sum(member, axis=0)
    list_sums, counts = lax.psum((list_sums, counts), "gy")
    average = list_sums / jnp.maximum(counts, 1.0)[:, None]
    own_columns = subspaces // lax.axis_size("gy")
    list_error = lax.dynamic_slice_in_dim(
        average, lax.axis_index("gy") * own_columns, own_columns, 1
    )
    return (quant_error, list_error)


def solution(mesh):
    in_specs = (
        P(("gx", "gy"), None),
        P(("gx", "gy")),
        P(),
        P(),
        P("gx", "gy"),
        P(),
        P("gy", None, None),
    )
    out_specs = (P(("gx", "gy"), None), P("gx", "gy"))
    return jax.shard_map(
        on_device, mesh=mesh, in_specs=in_specs, out_specs=out_specs, check_vma=False
    )
```

```python
import functools

import jax
import jax.numpy as jnp
from jax import lax
from jax.experimental import pallas as pl
from jax.experimental.pallas import tpu as pltpu
from jax.sharding import PartitionSpec as P

LANES = 128
WIDE = 2 * LANES
F32 = jnp.float32
BF16 = jnp.bfloat16


VMEM = pl.BlockSpec(memory_space=pltpu.VMEM)


def on_chip(array):
    return pltpu.with_memory_space_constraint(array, pltpu.VMEM)


def iota_f32(shape, axis):
    return lax.broadcasted_iota(jnp.int32, shape, axis).astype(F32)


def dot(a, b, contract=((1,), (0,))):
    return lax.dot_general(a, b, (contract, ((), ())), preferred_element_type=F32)


def slot_digits(ids_across, order_ref):
    found = jnp.zeros((LANES, LANES), F32)
    for block in range(order_ref.shape[0]):
        found = jnp.where(ids_across == order_ref[block : block + 1, :], float(block + 1), found)
    hit = (found > 0.0).astype(F32)
    block_of = (found - hit).astype(BF16)
    ones = jnp.ones((8, LANES), BF16)
    lanes = iota_f32((8, LANES), 1).astype(BF16)
    slot = dot(ones, block_of, ((1,), (1,))) * float(LANES) + dot(lanes, hit.astype(BF16), ((1,), (1,)))
    high = jnp.floor(slot * (1.0 / WIDE))
    return high, slot - high * WIDE


def prepare_kernel(
    own, ids_hbm, old_hbm, new_hbm, book_hbm, vec_hbm, rot_hbm, cent_hbm,
    turned_ref, digit_ref, code_ref, rot_ref, mine_ref, ids_ref, old_ref, new_ref, book_ref, vec_ref, arrived,
):
    first = lax.axis_index("gx") * own
    side = lax.axis_index("gy")
    moves = (
        (ids_hbm, ids_ref),
        (old_hbm, old_ref),
        (new_hbm, new_ref),
        (book_hbm.at[pl.ds(first, own)], book_ref),
        (vec_hbm, vec_ref),
        (rot_hbm, rot_ref),
        (cent_hbm.at[pl.ds(side * LANES, LANES)], mine_ref),
    )
    copies = [pltpu.make_async_copy(src, dst, arrived.at[n]) for n, (src, dst) in enumerate(moves)]
    for copy in copies:
        copy.start()
    for copy in copies[:3]:
        copy.wait()
    ids_across = jnp.broadcast_to(ids_ref[...], (LANES, LANES)).astype(F32).T.astype(jnp.int32)
    old_high, old_low = slot_digits(ids_across, old_ref)
    new_high, new_low = slot_digits(ids_across, new_ref)
    row = lax.broadcasted_iota(jnp.int32, (8, LANES), 0)
    digits = jnp.where(row == 0, old_high, jnp.where(row == 1, old_low, jnp.where(row == 2, new_high, new_low)))
    digit_ref[...] = digits.astype(BF16)
    copies[3].wait()
    codes = book_ref.shape[2]
    row = lax.broadcasted_iota(jnp.int32, (8, codes), 0)
    parts, tails = [], []
    for m in range(own):
        words = book_ref[m].astype(F32)
        zero = jnp.zeros_like(words)
        parts.append(jnp.concatenate([-2.0 * words if n == m else zero for n in range(own)], axis=1))
        norm = jnp.sum(words * words, axis=0, keepdims=True)
        top = norm.astype(BF16).astype(F32)
        middle = (norm - top).astype(BF16).astype(F32)
        low = norm - top - middle
        tails.append(jnp.where(row == 0, top, jnp.where(row == 1, middle, jnp.where(row == 2, low, 0.0))))
    parts.append(jnp.concatenate(tails, axis=1))
    code_ref[...] = jnp.concatenate(parts, axis=0).T.astype(BF16)
    copies[4].wait()
    copies[5].wait()
    turned_ref[...] = dot(vec_ref[...], rot_ref[...]).T.astype(BF16)
    copies[6].wait()


def pack_kernel(width, mine_ref, other_ref, rot_ref, turned_ref, digit_ref, out_ref):
    side = lax.axis_index("gy")
    half = mine_ref.shape[1]
    other = other_ref[pl.ds(side * LANES, LANES), :]
    rotated = dot(mine_ref[...], rot_ref[pl.ds(side * half, half), :])
    rotated += dot(other, rot_ref[pl.ds((1 - side) * half, half), :])
    cents = rotated.T
    vectors = turned_ref[...].astype(F32)
    digits = digit_ref[...].astype(F32)
    for device in range(out_ref.shape[0]):
        at = (device % 2) * half + (device // 2) * width
        for part in range(width // 4):
            rows = slice(at + 4 * part, at + 4 * part + 4)
            out_ref[device, part] = vectors[rows].astype(BF16)
            out_ref[device, width // 4 + part] = cents[rows].astype(BF16)
        out_ref[device, width // 2] = digits[0:4].astype(BF16)


def encode_kernel(own, sub_width, in_ref, code_ref, out_ref, table_ref, low_ref, square_ref):
    devices = in_ref.shape[0]
    tiles = devices // 2
    width = own * sub_width
    codes = code_ref.shape[0] // own

    def pair(tile, lo, hi):
        rows = []
        for part in range(lo // 4, hi // 4):
            rows.append(jnp.concatenate([in_ref[2 * tile, part], in_ref[2 * tile + 1, part]], axis=1).astype(F32))
        return jnp.concatenate(rows, axis=0) if len(rows) > 1 else rows[0]

    digits = [pair(tile, 2 * width, 2 * width + 4) for tile in range(tiles)]
    for tile in range(tiles):
        table_ref[tile * width : (tile + 1) * width, :] = pair(tile, width, 2 * width)
    table = table_ref[...].astype(BF16)
    sub = iota_f32((WIDE, WIDE), 0)
    tail_row = lax.broadcasted_iota(jnp.int32, (8, WIDE), 0)
    tail = (tail_row < 3).astype(F32)
    for tile in range(tiles):
        hot = (sub == digits[tile][1:2]).astype(F32).astype(BF16)
        looked = dot(table, hot)
        high = jnp.broadcast_to(digits[tile][0:1], (width, WIDE))
        cent = jnp.zeros((width, WIDE), F32)
        for group in range(tiles):
            cent = jnp.where(high == float(group), looked[group * width : (group + 1) * width], cent)
        turned = pair(tile, 0, width) - cent
        lanes = slice(tile * WIDE, (tile + 1) * WIDE)
        low_ref[:, lanes] = jnp.concatenate([turned, tail], axis=0).astype(BF16)
        squared = turned * turned
        for m in range(own):
            square_ref[m : m + 1, lanes] = jnp.sum(
                squared[m * sub_width : (m + 1) * sub_width], axis=0, keepdims=True
            )
    code = code_ref[...]
    sums = jnp.zeros((tiles * 8, WIDE), F32)
    errors = []
    for tile in range(tiles):
        lanes = slice(tile * WIDE, (tile + 1) * WIDE)
        distance = dot(code, low_ref[:, lanes])
        nearest = jnp.concatenate(
            [jnp.min(distance[m * codes : (m + 1) * codes], axis=0, keepdims=True) for m in range(own)], axis=0
        )
        error = nearest + square_ref[0:own, lanes]
        errors.append(error)
        top = error.astype(BF16).astype(F32)
        rest = error - top
        pad = jnp.zeros((8 - 2 * own - 1, WIDE), F32)
        group_rows = jnp.concatenate([top, rest, jnp.ones((1, WIDE), F32), pad], axis=0)
        high = jnp.broadcast_to(digits[tile][2:3], (8, WIDE))
        spread = jnp.concatenate(
            [jnp.where(high == float(group), group_rows, 0.0) for group in range(tiles)], axis=0
        ).astype(BF16)
        hot = (sub == digits[tile][3:4]).astype(F32).astype(BF16)
        sums = sums + dot(spread, hot, ((1,), (1,)))
    for tile in range(tiles):
        group = sums[tile * 8 : (tile + 1) * 8]
        total = group[0:own] + group[own : 2 * own]
        mean = total / jnp.maximum(group[2 * own : 2 * own + 1], 1.0)
        pad = jnp.zeros((out_ref.shape[2] - own, LANES), F32)
        for side in range(2):
            error = errors[tile][:, side * LANES : (side + 1) * LANES]
            for part, rows in enumerate((error, mean[:, :LANES], mean[:, LANES:])):
                out_ref[2 * tile + side, part] = jnp.concatenate([rows, pad], axis=0).astype(BF16)


def finish_kernel(own, in_ref, quant_ref, list_ref):
    tiles = in_ref.shape[0] // 2
    side = lax.axis_index("gy")
    for device in range(2 * tiles):
        at = ((device % 2) * tiles + device // 2) * own
        quant_ref[at : at + own, :] = in_ref[device, 0].astype(F32)[0:own]
    for tile in range(tiles):
        at = tile * own
        list_ref[at : at + own, 0:LANES] = in_ref[2 * tile + side, 1].astype(F32)[0:own]
        list_ref[at : at + own, LANES:WIDE] = in_ref[2 * tile + side, 2].astype(F32)[0:own]


def on_device_by_column(vectors, list_ids, old_order, new_order, centroids, rotation, codebook):
    owners, sides = lax.axis_size("gx"), lax.axis_size("gy")
    devices = owners * sides
    subspaces, sub_width, codes = codebook.shape
    own = subspaces // owners
    width = own * sub_width
    features = vectors.shape[1]
    total = subspaces * sides
    other = lax.ppermute(centroids, "gy", [(0, 1), (1, 0)])
    turned, digits, code, rotation, mine = pl.pallas_call(
        functools.partial(prepare_kernel, own),
        out_shape=(
            pltpu.VMEM((features, LANES), BF16),
            pltpu.VMEM((8, LANES), BF16),
            pltpu.VMEM((own * codes, width + 8), BF16),
            pltpu.VMEM(rotation.shape, BF16),
            pltpu.VMEM((LANES, centroids.shape[1]), BF16),
        ),
        in_specs=[pl.BlockSpec(memory_space=pl.ANY)] * 7,
        out_specs=(VMEM,) * 5,
        scratch_shapes=[
            pltpu.VMEM((1, LANES), jnp.int32),
            pltpu.VMEM((old_order.shape[0] // LANES, LANES), jnp.int32),
            pltpu.VMEM((old_order.shape[0] // LANES, LANES), jnp.int32),
            pltpu.VMEM((own, sub_width, codes), BF16),
            pltpu.VMEM((LANES, features), BF16),
            pltpu.SemaphoreType.DMA((7,)),
        ],
        name="prepare",
    )(
        list_ids.reshape(1, LANES),
        old_order.reshape(-1, LANES),
        new_order.reshape(-1, LANES),
        codebook,
        vectors,
        rotation,
        centroids,
    )
    outgoing = pl.pallas_call(
        functools.partial(pack_kernel, width),
        out_shape=pltpu.VMEM((devices, width // 2 + 1, 4, LANES), BF16),
        in_specs=[VMEM] * 5,
        out_specs=VMEM,
        name="pack",
    )(*(on_chip(array) for array in (mine, other, rotation, turned, digits)))
    incoming = lax.all_to_all(outgoing, ("gx", "gy"), split_axis=0, concat_axis=0, tiled=True)
    returning = pl.pallas_call(
        functools.partial(encode_kernel, own, sub_width),
        out_shape=pltpu.VMEM((devices, 3, 4, LANES), BF16),
        scratch_shapes=[
            pltpu.VMEM((owners * width, WIDE), F32),
            pltpu.VMEM((width + 8, devices * LANES), BF16),
            pltpu.VMEM((8, devices * LANES), F32),
        ],
        in_specs=[VMEM] * 2,
        out_specs=VMEM,
        name="encode",
    )(on_chip(incoming), on_chip(code))
    returned = lax.all_to_all(returning, ("gx", "gy"), split_axis=0, concat_axis=0, tiled=True)
    quant_error, list_error = pl.pallas_call(
        functools.partial(finish_kernel, own),
        out_shape=(
            jax.ShapeDtypeStruct((total, LANES), F32),
            jax.ShapeDtypeStruct((subspaces, WIDE), F32),
        ),
        in_specs=[VMEM],
        out_specs=(VMEM, VMEM),
        name="finish",
    )(on_chip(returned))
    return quant_error.T, list_error.T


def on_device(vectors, list_ids, old_order, new_order, centroids, rotation, codebook):
    owners, sides = lax.axis_size("gx"), lax.axis_size("gy")
    subspaces, sub_width, codes = codebook.shape
    own = subspaces // owners
    by_column = (
        sides == 2
        and own * owners == subspaces
        and 1 <= own <= 3
        and sub_width == 8
        and codes % LANES == 0
        and vectors.shape[0] == LANES
        and centroids.shape[0] == WIDE
        and old_order.shape[0] == owners * WIDE
        and owners <= WIDE
    )
    plan = on_device_by_column if by_column else on_device_by_owner
    return plan(vectors, list_ids, old_order, new_order, centroids, rotation, codebook)


def subspace_errors(turned, codewords, code_norm):
    row_count = turned.shape[0]
    subspaces, sub_width, code_count = codewords.shape
    group_size = 8
    group_count = subspaces // group_size
    lowered = turned.astype(jnp.bfloat16).reshape(row_count, group_count, group_size, sub_width)
    lowered = jnp.moveaxis(lowered, 1, 0)
    squares = jnp.sum(
        (turned * turned).reshape(row_count, group_count, group_size, sub_width), axis=3
    )
    squares = jnp.moveaxis(squares, 1, 0)
    book_groups = codewords.reshape(group_count, group_size, sub_width, code_count)
    norm_groups = code_norm.reshape(group_count, group_size, code_count)

    def one_group(operands):
        lowered_part, square_part, book_part, norm_part = operands
        inner_terms = jnp.einsum(
            "rgd,gdk->rgk", lowered_part, book_part, preferred_element_type=jnp.float32
        )
        inner_terms = lax.optimization_barrier(inner_terms.astype(jnp.bfloat16)).astype(jnp.float32)
        distance = square_part[:, :, None] - 2.0 * inner_terms + norm_part[None, :, :]
        return jnp.min(distance, axis=2)

    nearest = lax.map(one_group, (lowered, squares, book_groups, norm_groups))
    return jnp.moveaxis(nearest, 0, 1).reshape(row_count, subspaces)


def on_device_by_owner(vectors, list_ids, old_order, new_order, centroids, rotation, codebook):
    owners = lax.axis_size("gx")
    owner_index = lax.axis_index("gx")
    lists_own = centroids.shape[0]
    list_total = old_order.shape[0]
    rows_dev = vectors.shape[0]
    feature_width = vectors.shape[1]
    capacity = 5 * rows_dev // (2 * owners)
    own_lists = lax.dynamic_slice_in_dim(new_order, owner_index * lists_own, lists_own)
    select = (own_lists[:, None] == old_order[None, :]).astype(jnp.bfloat16)
    own_part = jnp.dot(
        select,
        lax.all_gather(centroids, "gx", axis=0, tiled=True),
        preferred_element_type=jnp.float32,
    )
    own_centroids = lax.all_gather(own_part.astype(jnp.bfloat16), "gy", axis=1, tiled=True)
    rot_cent = jnp.dot(own_centroids, rotation, preferred_element_type=jnp.float32)
    padded_cent = jnp.concatenate([rot_cent, jnp.zeros((1, feature_width), jnp.float32)], axis=0)
    codewords = lax.all_gather(codebook, "gy", axis=0, tiled=True)
    code_float = codewords.astype(jnp.float32)
    code_norm = jnp.sum(code_float * code_float, axis=1)
    subspaces = codewords.shape[0]
    slot_of = (
        jnp.zeros((list_total,), jnp.int32)
        .at[new_order]
        .set(jnp.arange(list_total, dtype=jnp.int32))
    )
    new_slot = slot_of[list_ids]
    dest_owner = new_slot // lists_own
    local_list = new_slot % lists_own
    owner_hits = (dest_owner[:, None] == jnp.arange(owners, dtype=jnp.int32)[None, :]).astype(
        jnp.int32
    )
    before = jnp.cumsum(owner_hits, axis=0) - owner_hits
    position = jnp.sum(before * owner_hits, axis=1)
    target = dest_owner * capacity + position
    labels_flat = jnp.full((owners * capacity,), lists_own, jnp.int32).at[target].set(local_list)
    outgoing = jnp.zeros((owners * capacity, feature_width), jnp.bfloat16).at[target].set(vectors)
    incoming = lax.all_to_all(
        outgoing.reshape(owners, capacity, feature_width),
        "gx",
        split_axis=0,
        concat_axis=0,
        tiled=True,
    )
    labels = lax.all_to_all(
        labels_flat.astype(jnp.bfloat16).reshape(owners, capacity),
        "gx",
        split_axis=0,
        concat_axis=0,
        tiled=True,
    )
    turned = jnp.dot(
        incoming.reshape(-1, feature_width), rotation, preferred_element_type=jnp.float32
    )
    finish_turned = turned
    label_rows = labels.reshape(-1).astype(jnp.int32)
    finish_turned = finish_turned - jnp.take(padded_cent, label_rows, axis=0)
    errors = subspace_errors(finish_turned, codewords, code_norm)
    results = errors.reshape(labels.shape[0], labels.shape[1], subspaces)
    returned = lax.all_to_all(results, "gx", split_axis=0, concat_axis=0, tiled=True)
    quant_error = returned.reshape(owners * capacity, subspaces)[target]
    label_rows = labels.reshape(-1).astype(jnp.int32)
    member = (label_rows[:, None] == jnp.arange(lists_own, dtype=jnp.int32)[None, :]).astype(
        jnp.float32
    )
    list_sums = jnp.einsum(
        "rl,rm->lm", member, results.reshape(-1, subspaces), precision=lax.Precision.HIGHEST
    )
    counts = jnp.sum(member, axis=0)
    list_sums, counts = lax.psum((list_sums, counts), "gy")
    average = list_sums / jnp.maximum(counts, 1.0)[:, None]
    own_columns = subspaces // lax.axis_size("gy")
    list_error = lax.dynamic_slice_in_dim(
        average, lax.axis_index("gy") * own_columns, own_columns, 1
    )
    return (quant_error, list_error)


def solution(mesh):
    in_specs = (
        P(("gx", "gy"), None),
        P(("gx", "gy")),
        P(),
        P(),
        P("gx", "gy"),
        P(),
        P("gy", None, None),
    )
    out_specs = (P(("gx", "gy"), None), P("gx", "gy"))
    return jax.shard_map(
        on_device, mesh=mesh, in_specs=in_specs, out_specs=out_specs, check_vma=False
    )
```

```python
import functools

import jax
import jax.numpy as jnp
from jax import lax
from jax.experimental import pallas as pl
from jax.experimental.pallas import tpu as pltpu
from jax.sharding import PartitionSpec as P

LANES = 128
WIDE = 2 * LANES
F32 = jnp.float32
BF16 = jnp.bfloat16


VMEM = pl.BlockSpec(memory_space=pltpu.VMEM)


def on_chip(array):
    return pltpu.with_memory_space_constraint(array, pltpu.VMEM)


def iota_f32(shape, axis):
    return lax.broadcasted_iota(jnp.int32, shape, axis).astype(F32)


def dot(a, b, contract=((1,), (0,))):
    return lax.dot_general(a, b, (contract, ((), ())), preferred_element_type=F32)


def pick_lanes(rows, index):
    along = lax.GatherDimensionNumbers(
        offset_dims=(),
        collapsed_slice_dims=(1,),
        start_index_map=(1,),
        operand_batching_dims=(0,),
        start_indices_batching_dims=(0,),
    )
    return lax.gather(
        rows, index[..., None], along, slice_sizes=(1, 1), mode=lax.GatherScatterMode.PROMISE_IN_BOUNDS
    )


def slot_digits(ids_across, order_ref):
    found = jnp.zeros((LANES, LANES), F32)
    for block in range(order_ref.shape[0]):
        found = jnp.where(ids_across == order_ref[block : block + 1, :], float(block + 1), found)
    hit = (found > 0.0).astype(F32)
    block_of = (found - hit).astype(BF16)
    ones = jnp.ones((8, LANES), BF16)
    lanes = iota_f32((8, LANES), 1).astype(BF16)
    slot = dot(ones, block_of, ((1,), (1,))) * float(LANES) + dot(lanes, hit.astype(BF16), ((1,), (1,)))
    high = jnp.floor(slot * (1.0 / WIDE))
    return high, slot - high * WIDE


def prepare_kernel(
    own, ids_hbm, old_hbm, new_hbm, book_hbm, vec_hbm, rot_hbm, cent_hbm,
    turned_ref, digit_ref, code_ref, rot_ref, mine_ref, ids_ref, old_ref, new_ref, book_ref, vec_ref, arrived,
):
    first = lax.axis_index("gx") * own
    side = lax.axis_index("gy")
    moves = (
        (ids_hbm, ids_ref),
        (old_hbm, old_ref),
        (new_hbm, new_ref),
        (book_hbm.at[pl.ds(first, own)], book_ref),
        (vec_hbm, vec_ref),
        (rot_hbm, rot_ref),
        (cent_hbm.at[pl.ds(side * LANES, LANES)], mine_ref),
    )
    copies = [pltpu.make_async_copy(src, dst, arrived.at[n]) for n, (src, dst) in enumerate(moves)]
    for copy in copies:
        copy.start()
    for copy in copies[:3]:
        copy.wait()
    ids_across = jnp.broadcast_to(ids_ref[...], (LANES, LANES)).astype(F32).T.astype(jnp.int32)
    old_high, old_low = slot_digits(ids_across, old_ref)
    new_high, new_low = slot_digits(ids_across, new_ref)
    row = lax.broadcasted_iota(jnp.int32, (8, LANES), 0)
    digits = jnp.where(row == 0, old_high, jnp.where(row == 1, old_low, jnp.where(row == 2, new_high, new_low)))
    digit_ref[...] = digits.astype(BF16)
    copies[3].wait()
    codes = book_ref.shape[2]
    row = lax.broadcasted_iota(jnp.int32, (8, codes), 0)
    parts, tails = [], []
    for m in range(own):
        words = book_ref[m].astype(F32)
        zero = jnp.zeros_like(words)
        parts.append(jnp.concatenate([-2.0 * words if n == m else zero for n in range(own)], axis=1))
        norm = jnp.sum(words * words, axis=0, keepdims=True)
        top = norm.astype(BF16).astype(F32)
        middle = (norm - top).astype(BF16).astype(F32)
        low = norm - top - middle
        tails.append(jnp.where(row == 0, top, jnp.where(row == 1, middle, jnp.where(row == 2, low, 0.0))))
    parts.append(jnp.concatenate(tails, axis=1))
    code_ref[...] = jnp.concatenate(parts, axis=0).T.astype(BF16)
    copies[4].wait()
    copies[5].wait()
    turned_ref[...] = dot(vec_ref[...], rot_ref[...]).T.astype(BF16)
    copies[6].wait()


def pack_kernel(width, mine_ref, other_ref, rot_ref, turned_ref, digit_ref, out_ref):
    side = lax.axis_index("gy")
    half = mine_ref.shape[1]
    other = other_ref[pl.ds(side * LANES, LANES), :]
    rotated = dot(mine_ref[...], rot_ref[pl.ds(side * half, half), :])
    rotated += dot(other, rot_ref[pl.ds((1 - side) * half, half), :])
    cents = rotated.T
    vectors = turned_ref[...].astype(F32)
    digits = digit_ref[...].astype(F32)
    for device in range(out_ref.shape[0]):
        at = (device % 2) * half + (device // 2) * width
        for part in range(width // 4):
            rows = slice(at + 4 * part, at + 4 * part + 4)
            out_ref[device, part] = vectors[rows].astype(BF16)
            out_ref[device, width // 4 + part] = cents[rows].astype(BF16)
        out_ref[device, width // 2] = digits[0:4].astype(BF16)


def encode_kernel(own, sub_width, in_ref, code_ref, out_ref, table_ref, low_ref):
    devices = in_ref.shape[0]
    tiles = devices // 2
    width = own * sub_width
    parts = width // 4
    codes = code_ref.shape[0] // own

    def stack(device, first):
        return jnp.concatenate([in_ref[device, first + n].astype(F32) for n in range(parts)], axis=0)

    digits = [in_ref[device, 2 * parts].astype(F32) for device in range(devices)]
    for tile in range(tiles):
        rows = jnp.concatenate([stack(2 * tile, parts), stack(2 * tile + 1, parts)], axis=0)
        table_ref[tile] = rows.astype(BF16)
    lane = lax.broadcasted_iota(jnp.int32, (WIDE, WIDE), 0).astype(F32)
    tail = (lax.broadcasted_iota(jnp.int32, (8, LANES), 0) < 3).astype(F32)
    code = code_ref[...]

    def turn(device):
        chunks = 2 * width // 16
        group = jnp.broadcast_to(digits[device][0:1], (16, LANES)).astype(BF16)
        place = digits[device][1:2]
        odd = place >= float(LANES)
        index = jnp.where(odd, place - float(LANES), place).astype(jnp.int32)
        index = jnp.broadcast_to(index, (16, LANES)).astype(jnp.int16)
        found = [jnp.zeros((16, LANES), BF16) for _ in range(chunks)]
        for tile in range(tiles):
            here = group == jnp.asarray(tile, BF16)
            for n in range(chunks):
                found[n] = jnp.where(here, pick_lanes(table_ref[tile, 16 * n : 16 * n + 16, :], index), found[n])
        both = jnp.concatenate([part.astype(F32) for part in found], axis=0)
        odd = jnp.broadcast_to(odd, (width, LANES))
        turned = stack(device, 0) - jnp.where(odd, both[width:], both[:width])
        low_ref[device] = jnp.concatenate([turned, tail], axis=0).astype(BF16)
        squared = turned * turned
        return jnp.concatenate(
            [jnp.sum(squared[8 * n : 8 * n + 8], axis=0, keepdims=True) for n in range(own)], axis=0
        )

    def measure(tile, squares):
        low = jnp.concatenate([low_ref[2 * tile], low_ref[2 * tile + 1]], axis=1)
        distance = dot(code, low)
        nearest = [jnp.min(distance[m * codes : (m + 1) * codes], axis=0, keepdims=True) for m in range(own)]
        return jnp.concatenate(nearest, axis=0) + jnp.concatenate(squares, axis=1)

    def gather(tile, error, sums):
        pair = jnp.concatenate([digits[2 * tile], digits[2 * tile + 1]], axis=1)
        top = error.astype(BF16).astype(F32)
        pad = jnp.zeros((8 - 2 * own - 1, WIDE), F32)
        for side in range(2):
            out_ref[2 * tile + side, 0] = jnp.concatenate([top, error - top], axis=0)[
                0:4, side * LANES : (side + 1) * LANES
            ].astype(BF16)
        rows = jnp.concatenate([top, error - top, jnp.ones((1, WIDE), F32), pad], axis=0)
        high = jnp.broadcast_to(pair[2:3], (8, WIDE))
        spread = jnp.concatenate([jnp.where(high == float(group), rows, 0.0) for group in range(tiles)], axis=0)
        hot = (pair[3:4] == lane).astype(F32).astype(BF16)
        return sums + dot(spread.astype(BF16), hot, ((1,), (1,)))

    sums = jnp.zeros((tiles * 8, WIDE), F32)
    errors = []
    squares = [turn(0), turn(1)]
    for tile in range(tiles):
        ahead = [turn(2 * tile + 2), turn(2 * tile + 3)] if tile + 1 < tiles else None
        errors.append(measure(tile, squares))
        if tile:
            sums = gather(tile - 1, errors[tile - 1], sums)
        squares = ahead
    sums = gather(tiles - 1, errors[tiles - 1], sums)
    for tile in range(tiles):
        group = sums[tile * 8 : (tile + 1) * 8]
        total = group[0:own] + group[own : 2 * own]
        mean = total / jnp.maximum(group[2 * own : 2 * own + 1], 1.0)
        pad = jnp.zeros((out_ref.shape[2] - own, LANES), F32)
        for side in range(2):
            for part, rows in enumerate((mean[:, :LANES], mean[:, LANES:])):
                out_ref[2 * tile + side, part + 1] = jnp.concatenate([rows, pad], axis=0).astype(BF16)


def finish_kernel(own, in_ref, quant_ref, list_ref):
    tiles = in_ref.shape[0] // 2
    side = lax.axis_index("gy")
    for device in range(2 * tiles):
        at = ((device % 2) * tiles + device // 2) * own
        quant_ref[at : at + own, :] = in_ref[device, 0].astype(F32)[0:own]
    for tile in range(tiles):
        at = tile * own
        list_ref[at : at + own, 0:LANES] = in_ref[2 * tile + side, 1].astype(F32)[0:own]
        list_ref[at : at + own, LANES:WIDE] = in_ref[2 * tile + side, 2].astype(F32)[0:own]


def on_device_by_column(vectors, list_ids, old_order, new_order, centroids, rotation, codebook):
    owners, sides = lax.axis_size("gx"), lax.axis_size("gy")
    devices = owners * sides
    subspaces, sub_width, codes = codebook.shape
    own = subspaces // owners
    width = own * sub_width
    features = vectors.shape[1]
    total = subspaces * sides
    other = lax.ppermute(centroids, "gy", [(0, 1), (1, 0)])
    turned, digits, code, rotation, mine = pl.pallas_call(
        functools.partial(prepare_kernel, own),
        out_shape=(
            pltpu.VMEM((features, LANES), BF16),
            pltpu.VMEM((8, LANES), BF16),
            pltpu.VMEM((own * codes, width + 8), BF16),
            pltpu.VMEM(rotation.shape, BF16),
            pltpu.VMEM((LANES, centroids.shape[1]), BF16),
        ),
        in_specs=[pl.BlockSpec(memory_space=pl.ANY)] * 7,
        out_specs=(VMEM,) * 5,
        scratch_shapes=[
            pltpu.VMEM((1, LANES), jnp.int32),
            pltpu.VMEM((old_order.shape[0] // LANES, LANES), jnp.int32),
            pltpu.VMEM((old_order.shape[0] // LANES, LANES), jnp.int32),
            pltpu.VMEM((own, sub_width, codes), BF16),
            pltpu.VMEM((LANES, features), BF16),
            pltpu.SemaphoreType.DMA((7,)),
        ],
        name="prepare",
    )(
        list_ids.reshape(1, LANES),
        old_order.reshape(-1, LANES),
        new_order.reshape(-1, LANES),
        codebook,
        vectors,
        rotation,
        centroids,
    )
    outgoing = pl.pallas_call(
        functools.partial(pack_kernel, width),
        out_shape=pltpu.VMEM((devices, width // 2 + 1, 4, LANES), BF16),
        in_specs=[VMEM] * 5,
        out_specs=VMEM,
        name="pack",
    )(*(on_chip(array) for array in (mine, other, rotation, turned, digits)))
    incoming = lax.all_to_all(outgoing, ("gx", "gy"), split_axis=0, concat_axis=0, tiled=True)
    returning = pl.pallas_call(
        functools.partial(encode_kernel, own, sub_width),
        out_shape=pltpu.VMEM((devices, 3, 4, LANES), BF16),
        scratch_shapes=[
            pltpu.VMEM((owners, 2 * width, LANES), BF16),
            pltpu.VMEM((devices, width + 8, LANES), BF16),
        ],
        in_specs=[VMEM] * 2,
        out_specs=VMEM,
        name="encode",
    )(on_chip(incoming), on_chip(code))
    returned = lax.all_to_all(returning, ("gx", "gy"), split_axis=0, concat_axis=0, tiled=True)
    quant_error, list_error = pl.pallas_call(
        functools.partial(finish_kernel, own),
        out_shape=(
            jax.ShapeDtypeStruct((total, LANES), F32),
            jax.ShapeDtypeStruct((subspaces, WIDE), F32),
        ),
        in_specs=[VMEM],
        out_specs=(VMEM, VMEM),
        name="finish",
    )(on_chip(returned))
    return quant_error.T, list_error.T


def on_device(vectors, list_ids, old_order, new_order, centroids, rotation, codebook):
    owners, sides = lax.axis_size("gx"), lax.axis_size("gy")
    subspaces, sub_width, codes = codebook.shape
    own = subspaces // owners
    by_column = (
        sides == 2
        and own * owners == subspaces
        and 1 <= own <= 3
        and sub_width == 8
        and codes % LANES == 0
        and vectors.shape[0] == LANES
        and centroids.shape[0] == WIDE
        and old_order.shape[0] == owners * WIDE
        and owners <= WIDE
    )
    plan = on_device_by_column if by_column else on_device_by_owner
    return plan(vectors, list_ids, old_order, new_order, centroids, rotation, codebook)


def subspace_errors(turned, codewords, code_norm):
    row_count = turned.shape[0]
    subspaces, sub_width, code_count = codewords.shape
    group_size = 8
    group_count = subspaces // group_size
    lowered = turned.astype(jnp.bfloat16).reshape(row_count, group_count, group_size, sub_width)
    lowered = jnp.moveaxis(lowered, 1, 0)
    squares = jnp.sum(
        (turned * turned).reshape(row_count, group_count, group_size, sub_width), axis=3
    )
    squares = jnp.moveaxis(squares, 1, 0)
    book_groups = codewords.reshape(group_count, group_size, sub_width, code_count)
    norm_groups = code_norm.reshape(group_count, group_size, code_count)

    def one_group(operands):
        lowered_part, square_part, book_part, norm_part = operands
        inner_terms = jnp.einsum(
            "rgd,gdk->rgk", lowered_part, book_part, preferred_element_type=jnp.float32
        )
        inner_terms = lax.optimization_barrier(inner_terms.astype(jnp.bfloat16)).astype(jnp.float32)
        distance = square_part[:, :, None] - 2.0 * inner_terms + norm_part[None, :, :]
        return jnp.min(distance, axis=2)

    nearest = lax.map(one_group, (lowered, squares, book_groups, norm_groups))
    return jnp.moveaxis(nearest, 0, 1).reshape(row_count, subspaces)


def on_device_by_owner(vectors, list_ids, old_order, new_order, centroids, rotation, codebook):
    owners = lax.axis_size("gx")
    owner_index = lax.axis_index("gx")
    lists_own = centroids.shape[0]
    list_total = old_order.shape[0]
    rows_dev = vectors.shape[0]
    feature_width = vectors.shape[1]
    capacity = 5 * rows_dev // (2 * owners)
    own_lists = lax.dynamic_slice_in_dim(new_order, owner_index * lists_own, lists_own)
    select = (own_lists[:, None] == old_order[None, :]).astype(jnp.bfloat16)
    own_part = jnp.dot(
        select,
        lax.all_gather(centroids, "gx", axis=0, tiled=True),
        preferred_element_type=jnp.float32,
    )
    own_centroids = lax.all_gather(own_part.astype(jnp.bfloat16), "gy", axis=1, tiled=True)
    rot_cent = jnp.dot(own_centroids, rotation, preferred_element_type=jnp.float32)
    padded_cent = jnp.concatenate([rot_cent, jnp.zeros((1, feature_width), jnp.float32)], axis=0)
    codewords = lax.all_gather(codebook, "gy", axis=0, tiled=True)
    code_float = codewords.astype(jnp.float32)
    code_norm = jnp.sum(code_float * code_float, axis=1)
    subspaces = codewords.shape[0]
    slot_of = (
        jnp.zeros((list_total,), jnp.int32)
        .at[new_order]
        .set(jnp.arange(list_total, dtype=jnp.int32))
    )
    new_slot = slot_of[list_ids]
    dest_owner = new_slot // lists_own
    local_list = new_slot % lists_own
    owner_hits = (dest_owner[:, None] == jnp.arange(owners, dtype=jnp.int32)[None, :]).astype(
        jnp.int32
    )
    before = jnp.cumsum(owner_hits, axis=0) - owner_hits
    position = jnp.sum(before * owner_hits, axis=1)
    target = dest_owner * capacity + position
    labels_flat = jnp.full((owners * capacity,), lists_own, jnp.int32).at[target].set(local_list)
    outgoing = jnp.zeros((owners * capacity, feature_width), jnp.bfloat16).at[target].set(vectors)
    incoming = lax.all_to_all(
        outgoing.reshape(owners, capacity, feature_width),
        "gx",
        split_axis=0,
        concat_axis=0,
        tiled=True,
    )
    labels = lax.all_to_all(
        labels_flat.astype(jnp.bfloat16).reshape(owners, capacity),
        "gx",
        split_axis=0,
        concat_axis=0,
        tiled=True,
    )
    turned = jnp.dot(
        incoming.reshape(-1, feature_width), rotation, preferred_element_type=jnp.float32
    )
    finish_turned = turned
    label_rows = labels.reshape(-1).astype(jnp.int32)
    finish_turned = finish_turned - jnp.take(padded_cent, label_rows, axis=0)
    errors = subspace_errors(finish_turned, codewords, code_norm)
    results = errors.reshape(labels.shape[0], labels.shape[1], subspaces)
    returned = lax.all_to_all(results, "gx", split_axis=0, concat_axis=0, tiled=True)
    quant_error = returned.reshape(owners * capacity, subspaces)[target]
    label_rows = labels.reshape(-1).astype(jnp.int32)
    member = (label_rows[:, None] == jnp.arange(lists_own, dtype=jnp.int32)[None, :]).astype(
        jnp.float32
    )
    list_sums = jnp.einsum(
        "rl,rm->lm", member, results.reshape(-1, subspaces), precision=lax.Precision.HIGHEST
    )
    counts = jnp.sum(member, axis=0)
    list_sums, counts = lax.psum((list_sums, counts), "gy")
    average = list_sums / jnp.maximum(counts, 1.0)[:, None]
    own_columns = subspaces // lax.axis_size("gy")
    list_error = lax.dynamic_slice_in_dim(
        average, lax.axis_index("gy") * own_columns, own_columns, 1
    )
    return (quant_error, list_error)


def solution(mesh):
    in_specs = (
        P(("gx", "gy"), None),
        P(("gx", "gy")),
        P(),
        P(),
        P("gx", "gy"),
        P(),
        P("gy", None, None),
    )
    out_specs = (P(("gx", "gy"), None), P("gx", "gy"))
    return jax.shard_map(
        on_device, mesh=mesh, in_specs=in_specs, out_specs=out_specs, check_vma=False
    )
```

```python
import functools

import jax
import jax.numpy as jnp
from jax import lax
from jax.experimental import pallas as pl
from jax.experimental.pallas import tpu as pltpu
from jax.sharding import PartitionSpec as P

LANES = 128
WIDE = 2 * LANES
F32 = jnp.float32
BF16 = jnp.bfloat16


VMEM = pl.BlockSpec(memory_space=pltpu.VMEM)


def on_chip(array):
    return pltpu.with_memory_space_constraint(array, pltpu.VMEM)


def iota_f32(shape, axis):
    return lax.broadcasted_iota(jnp.int32, shape, axis).astype(F32)


def dot(a, b, contract=((1,), (0,))):
    return lax.dot_general(a, b, (contract, ((), ())), preferred_element_type=F32)


def pick_lanes(rows, index):
    along = lax.GatherDimensionNumbers(
        offset_dims=(),
        collapsed_slice_dims=(1,),
        start_index_map=(1,),
        operand_batching_dims=(0,),
        start_indices_batching_dims=(0,),
    )
    return lax.gather(
        rows, index[..., None], along, slice_sizes=(1, 1), mode=lax.GatherScatterMode.PROMISE_IN_BOUNDS
    )


def slot_digits(ids_across, order_ref):
    order = order_ref[...].astype(jnp.int16)
    found = jnp.zeros((LANES, LANES), BF16)
    for block in range(order_ref.shape[0]):
        found = jnp.where(ids_across == order[block : block + 1, :], jnp.asarray(block + 1, BF16), found)
    found = found.astype(F32)
    hit = (found > 0.0).astype(F32)
    block_of = (found - hit).astype(BF16)
    ones = jnp.ones((8, LANES), BF16)
    lanes = iota_f32((8, LANES), 1).astype(BF16)
    slot = dot(ones, block_of, ((1,), (1,))) * float(LANES) + dot(lanes, hit.astype(BF16), ((1,), (1,)))
    high = jnp.floor(slot * (1.0 / WIDE))
    return high, slot - high * WIDE


def prepare_kernel(
    own, ids_hbm, old_hbm, new_hbm, vec_hbm, rot_hbm, cent_hbm, book_hbm,
    turned_ref, digit_ref, rot_ref, mine_ref, book_ref, ids_ref, old_ref, new_ref, vec_ref, arrived,
):
    side = lax.axis_index("gy")
    moves = (
        (ids_hbm, ids_ref),
        (old_hbm, old_ref),
        (new_hbm, new_ref),
        (vec_hbm, vec_ref),
        (rot_hbm, rot_ref),
        (cent_hbm.at[pl.ds(side * LANES, LANES)], mine_ref),
        (book_hbm.at[pl.ds(lax.axis_index("gx") * own, own)], book_ref),
    )
    copies = [pltpu.make_async_copy(src, dst, arrived.at[n]) for n, (src, dst) in enumerate(moves)]
    for copy in copies:
        copy.start()
    for copy in copies[:3]:
        copy.wait()
    ids_across = jnp.broadcast_to(ids_ref[...], (LANES, LANES)).astype(F32).T.astype(jnp.int32).astype(jnp.int16)
    old_high, old_low = slot_digits(ids_across, old_ref)
    new_high, new_low = slot_digits(ids_across, new_ref)
    row = lax.broadcasted_iota(jnp.int32, (8, LANES), 0)
    digits = jnp.where(row == 0, old_high, jnp.where(row == 1, old_low, jnp.where(row == 2, new_high, new_low)))
    digit_ref[...] = digits.astype(BF16)
    copies[3].wait()
    copies[4].wait()
    turned_ref[...] = dot(vec_ref[...], rot_ref[...]).T.astype(BF16)
    copies[5].wait()
    copies[6].wait()


def code_table(words):
    own = len(words)
    row = lax.broadcasted_iota(jnp.int32, words[0].shape, 0)
    parts, tails = [], []
    for m, word in enumerate(words):
        zero = jnp.zeros_like(word)
        parts.append(jnp.concatenate([-2.0 * word if n == m else zero for n in range(own)], axis=1))
        norm = jnp.sum(word * word, axis=0, keepdims=True)
        top = norm.astype(BF16).astype(F32)
        middle = (norm - top).astype(BF16).astype(F32)
        low = norm - top - middle
        tails.append(jnp.where(row == 0, top, jnp.where(row == 1, middle, jnp.where(row == 2, low, 0.0))))
    parts.append(jnp.concatenate(tails, axis=1))
    return jnp.concatenate(parts, axis=0).T.astype(BF16)


def pack_kernel(mine_ref, other_ref, rot_ref, turned_ref, digit_ref, book_ref, out_ref, code_ref):
    side = lax.axis_index("gy")
    half = mine_ref.shape[1]
    own, sub_width = book_ref.shape[:2]
    width = own * sub_width
    other = other_ref[pl.ds(side * LANES, LANES), :]
    rotated = dot(mine_ref[...], rot_ref[pl.ds(side * half, half), :])
    rotated += dot(other, rot_ref[pl.ds((1 - side) * half, half), :])
    code_ref[...] = code_table([book_ref[m].astype(F32) for m in range(own)])
    cents = rotated.T
    vectors = turned_ref[...].astype(F32)
    digits = digit_ref[...].astype(F32)
    for device in range(out_ref.shape[0]):
        for part in range(width // 4):
            at = (device % 2) * half + (device // 2) * width + 4 * part
            out_ref[device, part] = vectors[at : at + 4].astype(BF16)
            out_ref[device, width // 4 + part] = cents[at : at + 4].astype(BF16)
        out_ref[device, width // 2] = digits[0:4].astype(BF16)


def encode_kernel(own, sub_width, in_ref, code_ref, out_ref, table_ref, low_ref):
    devices = in_ref.shape[0]
    tiles = devices // 2
    width = own * sub_width
    parts = width // 4
    codes = code_ref.shape[0] // own

    def stack(device, first):
        return jnp.concatenate([in_ref[device, first + n].astype(F32) for n in range(parts)], axis=0)

    digits = [in_ref[device, 2 * parts].astype(F32) for device in range(devices)]
    for tile in range(tiles):
        rows = jnp.concatenate([stack(2 * tile, parts), stack(2 * tile + 1, parts)], axis=0)
        table_ref[tile] = rows.astype(BF16)
    lane = lax.broadcasted_iota(jnp.int32, (WIDE, WIDE), 0).astype(F32)
    tail = (lax.broadcasted_iota(jnp.int32, (8, LANES), 0) < 3).astype(F32)
    code = code_ref[...]

    def turn(device):
        chunks = 2 * width // 16
        group = jnp.broadcast_to(digits[device][0:1], (16, LANES)).astype(BF16)
        place = digits[device][1:2]
        odd = place >= float(LANES)
        index = jnp.where(odd, place - float(LANES), place).astype(jnp.int32)
        index = jnp.broadcast_to(index, (16, LANES)).astype(jnp.int16)
        found = [jnp.zeros((16, LANES), BF16) for _ in range(chunks)]
        for tile in range(tiles):
            here = group == jnp.asarray(tile, BF16)
            for n in range(chunks):
                found[n] = jnp.where(here, pick_lanes(table_ref[tile, 16 * n : 16 * n + 16, :], index), found[n])
        both = jnp.concatenate([part.astype(F32) for part in found], axis=0)
        odd = jnp.broadcast_to(odd, (width, LANES))
        turned = stack(device, 0) - jnp.where(odd, both[width:], both[:width])
        low_ref[device] = jnp.concatenate([turned, tail], axis=0).astype(BF16)
        squared = turned * turned
        return jnp.concatenate(
            [jnp.sum(squared[8 * n : 8 * n + 8], axis=0, keepdims=True) for n in range(own)], axis=0
        )

    def measure(tile, squares):
        low = jnp.concatenate([low_ref[2 * tile], low_ref[2 * tile + 1]], axis=1)
        distance = dot(code, low)
        nearest = [jnp.min(distance[m * codes : (m + 1) * codes], axis=0, keepdims=True) for m in range(own)]
        return jnp.concatenate(nearest, axis=0) + jnp.concatenate(squares, axis=1)

    def gather(tile, error, sums):
        pair = jnp.concatenate([digits[2 * tile], digits[2 * tile + 1]], axis=1)
        for side in range(2):
            out_ref[2 * tile + side, 0] = error[0:2, side * LANES : (side + 1) * LANES].astype(BF16)
        rows = jnp.concatenate([error, jnp.ones((1, WIDE), F32)] * 2, axis=0)
        high = jnp.broadcast_to(pair[2:3], (8, WIDE)) - upper
        spread = jnp.concatenate(
            [jnp.where(high == float(group), rows, 0.0) for group in range(0, tiles, 2)], axis=0
        )
        hot = (pair[3:4] == lane).astype(F32).astype(BF16)
        return sums + dot(spread.astype(BF16), hot, ((1,), (1,)))

    upper = (lax.broadcasted_iota(jnp.int32, (8, WIDE), 0) >= 4).astype(F32)
    sums = jnp.zeros((tiles * 4, WIDE), F32)
    errors = []
    squares = [turn(0), turn(1)]
    for tile in range(tiles):
        ahead = [turn(2 * tile + 2), turn(2 * tile + 3)] if tile + 1 < tiles else None
        errors.append(measure(tile, squares))
        if tile:
            sums = gather(tile - 1, errors[tile - 1], sums)
        squares = ahead
    sums = gather(tiles - 1, errors[tiles - 1], sums)
    spare = jnp.zeros((1, LANES), BF16)
    for tile in range(tiles):
        group = sums[tile * 4 : (tile + 1) * 4]
        mean = group[0:own] / jnp.maximum(group[own : own + 1], 1.0)
        left, right = mean[:, :LANES], mean[:, LANES:]
        last = jnp.concatenate([right[2:own].astype(BF16), spare], axis=0)
        for side in range(2):
            device = 2 * tile + side
            error = errors[tile][2:own, side * LANES : (side + 1) * LANES]
            out_ref[device, 1] = left[0:2].astype(BF16)
            out_ref[device, 2] = right[0:2].astype(BF16)
            out_ref[device, 3] = jnp.concatenate([error, left[2:own]], axis=0).astype(BF16)
            out_ref[device, 4] = last


def finish_kernel(own, in_ref, quant_ref, list_ref):
    tiles = in_ref.shape[0] // 2
    side = lax.axis_index("gy")
    for device in range(2 * tiles):
        at = ((device % 2) * tiles + device // 2) * own
        quant_ref[at : at + 2, :] = in_ref[device, 0].astype(F32)
        quant_ref[at + 2 : at + own, :] = in_ref[device, 3].astype(F32)[0:1]
    for tile in range(tiles):
        at, device = tile * own, 2 * tile + side
        list_ref[at : at + 2, 0:LANES] = in_ref[device, 1].astype(F32)
        list_ref[at : at + 2, LANES:WIDE] = in_ref[device, 2].astype(F32)
        list_ref[at + 2 : at + own, 0:LANES] = in_ref[device, 3].astype(F32)[1:2]
        list_ref[at + 2 : at + own, LANES:WIDE] = in_ref[device, 4].astype(F32)[0:1]


def on_device_by_column(vectors, list_ids, old_order, new_order, centroids, rotation, codebook):
    owners, sides = lax.axis_size("gx"), lax.axis_size("gy")
    devices = owners * sides
    subspaces, sub_width, codes = codebook.shape
    own = subspaces // owners
    width = own * sub_width
    features = vectors.shape[1]
    total = subspaces * sides
    other = lax.ppermute(centroids, "gy", [(0, 1), (1, 0)])
    turned, digits, rotation, mine, book = pl.pallas_call(
        functools.partial(prepare_kernel, own),
        out_shape=(
            pltpu.VMEM((features, LANES), BF16),
            pltpu.VMEM((8, LANES), BF16),
            pltpu.VMEM(rotation.shape, BF16),
            pltpu.VMEM((LANES, centroids.shape[1]), BF16),
            pltpu.VMEM((own, sub_width, codes), BF16),
        ),
        in_specs=[pl.BlockSpec(memory_space=pl.ANY)] * 7,
        out_specs=(VMEM,) * 5,
        scratch_shapes=[
            pltpu.VMEM((1, LANES), jnp.int32),
            pltpu.VMEM((old_order.shape[0] // LANES, LANES), jnp.int32),
            pltpu.VMEM((old_order.shape[0] // LANES, LANES), jnp.int32),
            pltpu.VMEM((LANES, features), BF16),
            pltpu.SemaphoreType.DMA((7,)),
        ],
        name="prepare",
    )(
        list_ids.reshape(1, LANES),
        old_order.reshape(-1, LANES),
        new_order.reshape(-1, LANES),
        vectors,
        rotation,
        centroids,
        codebook,
    )
    outgoing, code = pl.pallas_call(
        pack_kernel,
        out_shape=(
            pltpu.VMEM((devices, width // 2 + 1, 4, LANES), BF16),
            pltpu.VMEM((own * codes, width + 8), BF16),
        ),
        in_specs=[VMEM] * 6,
        out_specs=(VMEM, VMEM),
        name="pack",
    )(*(on_chip(array) for array in (mine, other, rotation, turned, digits, book)))
    incoming = lax.all_to_all(outgoing, ("gx", "gy"), split_axis=0, concat_axis=0, tiled=True)
    returning = pl.pallas_call(
        functools.partial(encode_kernel, own, sub_width),
        out_shape=pltpu.VMEM((devices, 5, 2, LANES), BF16),
        scratch_shapes=[
            pltpu.VMEM((owners, 2 * width, LANES), BF16),
            pltpu.VMEM((devices, width + 8, LANES), BF16),
        ],
        in_specs=[VMEM] * 2,
        out_specs=VMEM,
        name="encode",
    )(on_chip(incoming), on_chip(code))
    returned = lax.all_to_all(returning, ("gx", "gy"), split_axis=0, concat_axis=0, tiled=True)
    quant_error, list_error = pl.pallas_call(
        functools.partial(finish_kernel, own),
        out_shape=(
            jax.ShapeDtypeStruct((total, LANES), F32),
            jax.ShapeDtypeStruct((subspaces, WIDE), F32),
        ),
        in_specs=[VMEM],
        out_specs=(VMEM, VMEM),
        name="finish",
    )(on_chip(returned))
    return quant_error.T, list_error.T


def on_device(vectors, list_ids, old_order, new_order, centroids, rotation, codebook):
    owners, sides = lax.axis_size("gx"), lax.axis_size("gy")
    subspaces, sub_width, codes = codebook.shape
    own = subspaces // owners
    by_column = (
        sides == 2
        and own * owners == subspaces
        and own == 3
        and sub_width == 8
        and codes % LANES == 0
        and vectors.shape[0] == LANES
        and centroids.shape[0] == WIDE
        and old_order.shape[0] == owners * WIDE
        and owners <= WIDE
    )
    plan = on_device_by_column if by_column else on_device_by_owner
    return plan(vectors, list_ids, old_order, new_order, centroids, rotation, codebook)


def subspace_errors(turned, codewords, code_norm):
    row_count = turned.shape[0]
    subspaces, sub_width, code_count = codewords.shape
    group_size = 8
    group_count = subspaces // group_size
    lowered = turned.astype(jnp.bfloat16).reshape(row_count, group_count, group_size, sub_width)
    lowered = jnp.moveaxis(lowered, 1, 0)
    squares = jnp.sum(
        (turned * turned).reshape(row_count, group_count, group_size, sub_width), axis=3
    )
    squares = jnp.moveaxis(squares, 1, 0)
    book_groups = codewords.reshape(group_count, group_size, sub_width, code_count)
    norm_groups = code_norm.reshape(group_count, group_size, code_count)

    def one_group(operands):
        lowered_part, square_part, book_part, norm_part = operands
        inner_terms = jnp.einsum(
            "rgd,gdk->rgk", lowered_part, book_part, preferred_element_type=jnp.float32
        )
        inner_terms = lax.optimization_barrier(inner_terms.astype(jnp.bfloat16)).astype(jnp.float32)
        distance = square_part[:, :, None] - 2.0 * inner_terms + norm_part[None, :, :]
        return jnp.min(distance, axis=2)

    nearest = lax.map(one_group, (lowered, squares, book_groups, norm_groups))
    return jnp.moveaxis(nearest, 0, 1).reshape(row_count, subspaces)


def on_device_by_owner(vectors, list_ids, old_order, new_order, centroids, rotation, codebook):
    owners = lax.axis_size("gx")
    owner_index = lax.axis_index("gx")
    lists_own = centroids.shape[0]
    list_total = old_order.shape[0]
    rows_dev = vectors.shape[0]
    feature_width = vectors.shape[1]
    capacity = 5 * rows_dev // (2 * owners)
    own_lists = lax.dynamic_slice_in_dim(new_order, owner_index * lists_own, lists_own)
    select = (own_lists[:, None] == old_order[None, :]).astype(jnp.bfloat16)
    own_part = jnp.dot(
        select,
        lax.all_gather(centroids, "gx", axis=0, tiled=True),
        preferred_element_type=jnp.float32,
    )
    own_centroids = lax.all_gather(own_part.astype(jnp.bfloat16), "gy", axis=1, tiled=True)
    rot_cent = jnp.dot(own_centroids, rotation, preferred_element_type=jnp.float32)
    padded_cent = jnp.concatenate([rot_cent, jnp.zeros((1, feature_width), jnp.float32)], axis=0)
    codewords = lax.all_gather(codebook, "gy", axis=0, tiled=True)
    code_float = codewords.astype(jnp.float32)
    code_norm = jnp.sum(code_float * code_float, axis=1)
    subspaces = codewords.shape[0]
    slot_of = (
        jnp.zeros((list_total,), jnp.int32)
        .at[new_order]
        .set(jnp.arange(list_total, dtype=jnp.int32))
    )
    new_slot = slot_of[list_ids]
    dest_owner = new_slot // lists_own
    local_list = new_slot % lists_own
    owner_hits = (dest_owner[:, None] == jnp.arange(owners, dtype=jnp.int32)[None, :]).astype(
        jnp.int32
    )
    before = jnp.cumsum(owner_hits, axis=0) - owner_hits
    position = jnp.sum(before * owner_hits, axis=1)
    target = dest_owner * capacity + position
    labels_flat = jnp.full((owners * capacity,), lists_own, jnp.int32).at[target].set(local_list)
    outgoing = jnp.zeros((owners * capacity, feature_width), jnp.bfloat16).at[target].set(vectors)
    incoming = lax.all_to_all(
        outgoing.reshape(owners, capacity, feature_width),
        "gx",
        split_axis=0,
        concat_axis=0,
        tiled=True,
    )
    labels = lax.all_to_all(
        labels_flat.astype(jnp.bfloat16).reshape(owners, capacity),
        "gx",
        split_axis=0,
        concat_axis=0,
        tiled=True,
    )
    turned = jnp.dot(
        incoming.reshape(-1, feature_width), rotation, preferred_element_type=jnp.float32
    )
    finish_turned = turned
    label_rows = labels.reshape(-1).astype(jnp.int32)
    finish_turned = finish_turned - jnp.take(padded_cent, label_rows, axis=0)
    errors = subspace_errors(finish_turned, codewords, code_norm)
    results = errors.reshape(labels.shape[0], labels.shape[1], subspaces)
    returned = lax.all_to_all(results, "gx", split_axis=0, concat_axis=0, tiled=True)
    quant_error = returned.reshape(owners * capacity, subspaces)[target]
    label_rows = labels.reshape(-1).astype(jnp.int32)
    member = (label_rows[:, None] == jnp.arange(lists_own, dtype=jnp.int32)[None, :]).astype(
        jnp.float32
    )
    list_sums = jnp.einsum(
        "rl,rm->lm", member, results.reshape(-1, subspaces), precision=lax.Precision.HIGHEST
    )
    counts = jnp.sum(member, axis=0)
    list_sums, counts = lax.psum((list_sums, counts), "gy")
    average = list_sums / jnp.maximum(counts, 1.0)[:, None]
    own_columns = subspaces // lax.axis_size("gy")
    list_error = lax.dynamic_slice_in_dim(
        average, lax.axis_index("gy") * own_columns, own_columns, 1
    )
    return (quant_error, list_error)


def solution(mesh):
    in_specs = (
        P(("gx", "gy"), None),
        P(("gx", "gy")),
        P(),
        P(),
        P("gx", "gy"),
        P(),
        P("gy", None, None),
    )
    out_specs = (P(("gx", "gy"), None), P("gx", "gy"))
    return jax.shard_map(
        on_device, mesh=mesh, in_specs=in_specs, out_specs=out_specs, check_vma=False
    )
```

```python
import functools

import jax
import jax.numpy as jnp
from jax import lax
from jax.experimental import pallas as pl
from jax.experimental.pallas import tpu as pltpu
from jax.sharding import PartitionSpec as P

LANES = 128
WIDE = 2 * LANES
F32 = jnp.float32
BF16 = jnp.bfloat16


VMEM = pl.BlockSpec(memory_space=pltpu.VMEM)


def on_chip(array):
    return pltpu.with_memory_space_constraint(array, pltpu.VMEM)


def iota_f32(shape, axis):
    return lax.broadcasted_iota(jnp.int32, shape, axis).astype(F32)


def dot(a, b, contract=((1,), (0,))):
    return lax.dot_general(a, b, (contract, ((), ())), preferred_element_type=F32)


def pick_lanes(rows, index):
    along = lax.GatherDimensionNumbers(
        offset_dims=(),
        collapsed_slice_dims=(1,),
        start_index_map=(1,),
        operand_batching_dims=(0,),
        start_indices_batching_dims=(0,),
    )
    return lax.gather(
        rows, index[..., None], along, slice_sizes=(1, 1), mode=lax.GatherScatterMode.PROMISE_IN_BOUNDS
    )


def slot_digits(ids_across, order_ref):
    order = order_ref[...].astype(jnp.int16)
    found = jnp.zeros((LANES, LANES), BF16)
    for block in range(order_ref.shape[0]):
        found = jnp.where(ids_across == order[block : block + 1, :], jnp.asarray(block + 1, BF16), found)
    found = found.astype(F32)
    hit = (found > 0.0).astype(F32)
    block_of = (found - hit).astype(BF16)
    ones = jnp.ones((8, LANES), BF16)
    lanes = iota_f32((8, LANES), 1).astype(BF16)
    slot = dot(ones, block_of, ((1,), (1,))) * float(LANES) + dot(lanes, hit.astype(BF16), ((1,), (1,)))
    high = jnp.floor(slot * (1.0 / WIDE))
    return high, slot - high * WIDE


def prepare_kernel(
    own, ids_hbm, old_hbm, new_hbm, vec_hbm, rot_hbm, cent_hbm, book_hbm,
    vec_ref, digit_ref, rot_ref, mine_ref, book_ref, ids_ref, old_ref, new_ref, arrived,
):
    side = lax.axis_index("gy")
    moves = (
        (ids_hbm, ids_ref),
        (old_hbm, old_ref),
        (new_hbm, new_ref),
        (rot_hbm, rot_ref),
        (vec_hbm, vec_ref),
        (cent_hbm.at[pl.ds(side * LANES, LANES)], mine_ref),
        (book_hbm.at[pl.ds(lax.axis_index("gx") * own, own)], book_ref),
    )
    copies = [pltpu.make_async_copy(src, dst, arrived.at[n]) for n, (src, dst) in enumerate(moves)]
    for copy in copies:
        copy.start()
    for copy in copies[:3]:
        copy.wait()
    ids_across = jnp.broadcast_to(ids_ref[...], (LANES, LANES)).astype(F32).T.astype(jnp.int32).astype(jnp.int16)
    old_high, old_low = slot_digits(ids_across, old_ref)
    new_high, new_low = slot_digits(ids_across, new_ref)
    row = lax.broadcasted_iota(jnp.int32, (8, LANES), 0)
    digits = jnp.where(row == 0, old_high, jnp.where(row == 1, old_low, jnp.where(row == 2, new_high, new_low)))
    digit_ref[...] = digits.astype(BF16)
    for copy in copies[3:]:
        copy.wait()


def code_table(words):
    own = len(words)
    row = lax.broadcasted_iota(jnp.int32, words[0].shape, 0)
    parts, tails = [], []
    for m, word in enumerate(words):
        zero = jnp.zeros_like(word)
        parts.append(jnp.concatenate([-2.0 * word if n == m else zero for n in range(own)], axis=1))
        norm = jnp.sum(word * word, axis=0, keepdims=True)
        top = norm.astype(BF16).astype(F32)
        middle = (norm - top).astype(BF16).astype(F32)
        low = norm - top - middle
        tails.append(jnp.where(row == 0, top, jnp.where(row == 1, middle, jnp.where(row == 2, low, 0.0))))
    parts.append(jnp.concatenate(tails, axis=1))
    return jnp.concatenate(parts, axis=0).T.astype(BF16)


def pack_kernel(mine_ref, other_ref, rot_ref, vec_ref, digit_ref, book_ref, out_ref, code_ref):
    side = lax.axis_index("gy")
    half = mine_ref.shape[1]
    own, sub_width = book_ref.shape[:2]
    width = own * sub_width
    rotated = jnp.zeros((2 * LANES, rot_ref.shape[1]), F32)
    for at, cents in ((side, mine_ref[...]), (1 - side, other_ref[pl.ds(side * LANES, LANES), :])):
        rows = jnp.concatenate([vec_ref[:, pl.ds(at * half, half)], cents], axis=0)
        rotated += dot(rows, rot_ref[pl.ds(at * half, half), :])
    code_ref[...] = code_table([book_ref[m].astype(F32) for m in range(own)])
    turned = rotated.T
    vectors, cents = turned[:, :LANES], turned[:, LANES:]
    digits = digit_ref[...].astype(F32)
    for device in range(out_ref.shape[0]):
        for part in range(width // 4):
            at = (device % 2) * half + (device // 2) * width + 4 * part
            out_ref[device, part] = vectors[at : at + 4].astype(BF16)
            out_ref[device, width // 4 + part] = cents[at : at + 4].astype(BF16)
        out_ref[device, width // 2] = digits[0:4].astype(BF16)


def encode_kernel(own, sub_width, in_ref, code_ref, out_ref, table_ref, low_ref):
    devices = in_ref.shape[0]
    tiles = devices // 2
    width = own * sub_width
    parts = width // 4
    codes = code_ref.shape[0] // own

    def stack(device, first):
        return jnp.concatenate([in_ref[device, first + n].astype(F32) for n in range(parts)], axis=0)

    digits = [in_ref[device, 2 * parts].astype(F32) for device in range(devices)]
    for tile in range(tiles):
        rows = jnp.concatenate([stack(2 * tile, parts), stack(2 * tile + 1, parts)], axis=0)
        table_ref[tile] = rows.astype(BF16)
    lane = lax.broadcasted_iota(jnp.int32, (WIDE, WIDE), 0).astype(F32)
    tail = (lax.broadcasted_iota(jnp.int32, (8, LANES), 0) < 3).astype(F32)
    code = code_ref[...]

    def turn(device):
        chunks = 2 * width // 16
        group = jnp.broadcast_to(digits[device][0:1], (16, LANES)).astype(BF16)
        place = digits[device][1:2]
        odd = place >= float(LANES)
        index = jnp.where(odd, place - float(LANES), place).astype(jnp.int32)
        index = jnp.broadcast_to(index, (16, LANES)).astype(jnp.int16)
        found = [jnp.zeros((16, LANES), BF16) for _ in range(chunks)]
        for tile in range(tiles):
            here = group == jnp.asarray(tile, BF16)
            for n in range(chunks):
                found[n] = jnp.where(here, pick_lanes(table_ref[tile, 16 * n : 16 * n + 16, :], index), found[n])
        both = jnp.concatenate([part.astype(F32) for part in found], axis=0)
        odd = jnp.broadcast_to(odd, (width, LANES))
        turned = stack(device, 0) - jnp.where(odd, both[width:], both[:width])
        low_ref[device] = jnp.concatenate([turned, tail], axis=0).astype(BF16)
        squared = turned * turned
        return jnp.concatenate(
            [jnp.sum(squared[8 * n : 8 * n + 8], axis=0, keepdims=True) for n in range(own)], axis=0
        )

    def measure(tile, squares):
        low = jnp.concatenate([low_ref[2 * tile], low_ref[2 * tile + 1]], axis=1)
        distance = dot(code, low)
        nearest = [jnp.min(distance[m * codes : (m + 1) * codes], axis=0, keepdims=True) for m in range(own)]
        return jnp.concatenate(nearest, axis=0) + jnp.concatenate(squares, axis=1)

    def gather(tile, error, sums):
        pair = jnp.concatenate([digits[2 * tile], digits[2 * tile + 1]], axis=1)
        for side in range(2):
            out_ref[2 * tile + side, 0] = error[0:2, side * LANES : (side + 1) * LANES].astype(BF16)
        rows = jnp.concatenate([error, jnp.ones((1, WIDE), F32)] * 2, axis=0)
        high = jnp.broadcast_to(pair[2:3], (8, WIDE)) - upper
        spread = jnp.concatenate(
            [jnp.where(high == float(group), rows, 0.0) for group in range(0, tiles, 2)], axis=0
        )
        hot = (pair[3:4] == lane).astype(F32).astype(BF16)
        return sums + dot(spread.astype(BF16), hot, ((1,), (1,)))

    upper = (lax.broadcasted_iota(jnp.int32, (8, WIDE), 0) >= 4).astype(F32)
    sums = jnp.zeros((tiles * 4, WIDE), F32)
    errors = []
    squares = [turn(0), turn(1)]
    for tile in range(tiles):
        ahead = [turn(2 * tile + 2), turn(2 * tile + 3)] if tile + 1 < tiles else None
        errors.append(measure(tile, squares))
        if tile:
            sums = gather(tile - 1, errors[tile - 1], sums)
        squares = ahead
    sums = gather(tiles - 1, errors[tiles - 1], sums)
    spare = jnp.zeros((1, LANES), BF16)
    for tile in range(tiles):
        group = sums[tile * 4 : (tile + 1) * 4]
        mean = group[0:own] / jnp.maximum(group[own : own + 1], 1.0)
        left, right = mean[:, :LANES], mean[:, LANES:]
        last = jnp.concatenate([right[2:own].astype(BF16), spare], axis=0)
        for side in range(2):
            device = 2 * tile + side
            error = errors[tile][2:own, side * LANES : (side + 1) * LANES]
            out_ref[device, 1] = left[0:2].astype(BF16)
            out_ref[device, 2] = right[0:2].astype(BF16)
            out_ref[device, 3] = jnp.concatenate([error, left[2:own]], axis=0).astype(BF16)
            out_ref[device, 4] = last


def finish_kernel(own, in_ref, quant_ref, list_ref):
    tiles = in_ref.shape[0] // 2
    side = lax.axis_index("gy")
    for device in range(2 * tiles):
        at = ((device % 2) * tiles + device // 2) * own
        quant_ref[at : at + 2, :] = in_ref[device, 0].astype(F32)
        quant_ref[at + 2 : at + own, :] = in_ref[device, 3].astype(F32)[0:1]
    for tile in range(tiles):
        at, device = tile * own, 2 * tile + side
        list_ref[at : at + 2, 0:LANES] = in_ref[device, 1].astype(F32)
        list_ref[at : at + 2, LANES:WIDE] = in_ref[device, 2].astype(F32)
        list_ref[at + 2 : at + own, 0:LANES] = in_ref[device, 3].astype(F32)[1:2]
        list_ref[at + 2 : at + own, LANES:WIDE] = in_ref[device, 4].astype(F32)[0:1]


def on_device_by_column(vectors, list_ids, old_order, new_order, centroids, rotation, codebook):
    owners, sides = lax.axis_size("gx"), lax.axis_size("gy")
    devices = owners * sides
    subspaces, sub_width, codes = codebook.shape
    own = subspaces // owners
    width = own * sub_width
    features = vectors.shape[1]
    total = subspaces * sides
    other = lax.ppermute(centroids, "gy", [(0, 1), (1, 0)])
    vectors, digits, rotation, mine, book = pl.pallas_call(
        functools.partial(prepare_kernel, own),
        out_shape=(
            pltpu.VMEM((LANES, features), BF16),
            pltpu.VMEM((8, LANES), BF16),
            pltpu.VMEM(rotation.shape, BF16),
            pltpu.VMEM((LANES, centroids.shape[1]), BF16),
            pltpu.VMEM((own, sub_width, codes), BF16),
        ),
        in_specs=[pl.BlockSpec(memory_space=pl.ANY)] * 7,
        out_specs=(VMEM,) * 5,
        scratch_shapes=[
            pltpu.VMEM((1, LANES), jnp.int32),
            pltpu.VMEM((old_order.shape[0] // LANES, LANES), jnp.int32),
            pltpu.VMEM((old_order.shape[0] // LANES, LANES), jnp.int32),
            pltpu.SemaphoreType.DMA((7,)),
        ],
        name="prepare",
    )(
        list_ids.reshape(1, LANES),
        old_order.reshape(-1, LANES),
        new_order.reshape(-1, LANES),
        vectors,
        rotation,
        centroids,
        codebook,
    )
    outgoing, code = pl.pallas_call(
        pack_kernel,
        out_shape=(
            pltpu.VMEM((devices, width // 2 + 1, 4, LANES), BF16),
            pltpu.VMEM((own * codes, width + 8), BF16),
        ),
        in_specs=[VMEM] * 6,
        out_specs=(VMEM, VMEM),
        name="pack",
    )(*(on_chip(array) for array in (mine, other, rotation, vectors, digits, book)))
    incoming = lax.all_to_all(outgoing, ("gx", "gy"), split_axis=0, concat_axis=0, tiled=True)
    returning = pl.pallas_call(
        functools.partial(encode_kernel, own, sub_width),
        out_shape=pltpu.VMEM((devices, 5, 2, LANES), BF16),
        scratch_shapes=[
            pltpu.VMEM((owners, 2 * width, LANES), BF16),
            pltpu.VMEM((devices, width + 8, LANES), BF16),
        ],
        in_specs=[VMEM] * 2,
        out_specs=VMEM,
        name="encode",
    )(on_chip(incoming), on_chip(code))
    returned = lax.all_to_all(returning, ("gx", "gy"), split_axis=0, concat_axis=0, tiled=True)
    quant_error, list_error = pl.pallas_call(
        functools.partial(finish_kernel, own),
        out_shape=(
            jax.ShapeDtypeStruct((total, LANES), F32),
            jax.ShapeDtypeStruct((subspaces, WIDE), F32),
        ),
        in_specs=[VMEM],
        out_specs=(VMEM, VMEM),
        name="finish",
    )(on_chip(returned))
    return quant_error.T, list_error.T


def on_device(vectors, list_ids, old_order, new_order, centroids, rotation, codebook):
    owners, sides = lax.axis_size("gx"), lax.axis_size("gy")
    subspaces, sub_width, codes = codebook.shape
    own = subspaces // owners
    by_column = (
        sides == 2
        and own * owners == subspaces
        and own == 3
        and sub_width == 8
        and codes % LANES == 0
        and vectors.shape[0] == LANES
        and centroids.shape[0] == WIDE
        and old_order.shape[0] == owners * WIDE
        and owners <= LANES
        and owners % 2 == 0
    )
    plan = on_device_by_column if by_column else on_device_by_owner
    return plan(vectors, list_ids, old_order, new_order, centroids, rotation, codebook)


def subspace_errors(turned, codewords, code_norm):
    row_count = turned.shape[0]
    subspaces, sub_width, code_count = codewords.shape
    group_size = 8
    group_count = subspaces // group_size
    lowered = turned.astype(jnp.bfloat16).reshape(row_count, group_count, group_size, sub_width)
    lowered = jnp.moveaxis(lowered, 1, 0)
    squares = jnp.sum(
        (turned * turned).reshape(row_count, group_count, group_size, sub_width), axis=3
    )
    squares = jnp.moveaxis(squares, 1, 0)
    book_groups = codewords.reshape(group_count, group_size, sub_width, code_count)
    norm_groups = code_norm.reshape(group_count, group_size, code_count)

    def one_group(operands):
        lowered_part, square_part, book_part, norm_part = operands
        inner_terms = jnp.einsum(
            "rgd,gdk->rgk", lowered_part, book_part, preferred_element_type=jnp.float32
        )
        inner_terms = lax.optimization_barrier(inner_terms.astype(jnp.bfloat16)).astype(jnp.float32)
        distance = square_part[:, :, None] - 2.0 * inner_terms + norm_part[None, :, :]
        return jnp.min(distance, axis=2)

    nearest = lax.map(one_group, (lowered, squares, book_groups, norm_groups))
    return jnp.moveaxis(nearest, 0, 1).reshape(row_count, subspaces)


def on_device_by_owner(vectors, list_ids, old_order, new_order, centroids, rotation, codebook):
    owners = lax.axis_size("gx")
    owner_index = lax.axis_index("gx")
    lists_own = centroids.shape[0]
    list_total = old_order.shape[0]
    rows_dev = vectors.shape[0]
    feature_width = vectors.shape[1]
    capacity = 5 * rows_dev // (2 * owners)
    own_lists = lax.dynamic_slice_in_dim(new_order, owner_index * lists_own, lists_own)
    select = (own_lists[:, None] == old_order[None, :]).astype(jnp.bfloat16)
    own_part = jnp.dot(
        select,
        lax.all_gather(centroids, "gx", axis=0, tiled=True),
        preferred_element_type=jnp.float32,
    )
    own_centroids = lax.all_gather(own_part.astype(jnp.bfloat16), "gy", axis=1, tiled=True)
    rot_cent = jnp.dot(own_centroids, rotation, preferred_element_type=jnp.float32)
    padded_cent = jnp.concatenate([rot_cent, jnp.zeros((1, feature_width), jnp.float32)], axis=0)
    codewords = lax.all_gather(codebook, "gy", axis=0, tiled=True)
    code_float = codewords.astype(jnp.float32)
    code_norm = jnp.sum(code_float * code_float, axis=1)
    subspaces = codewords.shape[0]
    slot_of = (
        jnp.zeros((list_total,), jnp.int32)
        .at[new_order]
        .set(jnp.arange(list_total, dtype=jnp.int32))
    )
    new_slot = slot_of[list_ids]
    dest_owner = new_slot // lists_own
    local_list = new_slot % lists_own
    owner_hits = (dest_owner[:, None] == jnp.arange(owners, dtype=jnp.int32)[None, :]).astype(
        jnp.int32
    )
    before = jnp.cumsum(owner_hits, axis=0) - owner_hits
    position = jnp.sum(before * owner_hits, axis=1)
    target = dest_owner * capacity + position
    labels_flat = jnp.full((owners * capacity,), lists_own, jnp.int32).at[target].set(local_list)
    outgoing = jnp.zeros((owners * capacity, feature_width), jnp.bfloat16).at[target].set(vectors)
    incoming = lax.all_to_all(
        outgoing.reshape(owners, capacity, feature_width),
        "gx",
        split_axis=0,
        concat_axis=0,
        tiled=True,
    )
    labels = lax.all_to_all(
        labels_flat.astype(jnp.bfloat16).reshape(owners, capacity),
        "gx",
        split_axis=0,
        concat_axis=0,
        tiled=True,
    )
    turned = jnp.dot(
        incoming.reshape(-1, feature_width), rotation, preferred_element_type=jnp.float32
    )
    finish_turned = turned
    label_rows = labels.reshape(-1).astype(jnp.int32)
    finish_turned = finish_turned - jnp.take(padded_cent, label_rows, axis=0)
    errors = subspace_errors(finish_turned, codewords, code_norm)
    results = errors.reshape(labels.shape[0], labels.shape[1], subspaces)
    returned = lax.all_to_all(results, "gx", split_axis=0, concat_axis=0, tiled=True)
    quant_error = returned.reshape(owners * capacity, subspaces)[target]
    label_rows = labels.reshape(-1).astype(jnp.int32)
    member = (label_rows[:, None] == jnp.arange(lists_own, dtype=jnp.int32)[None, :]).astype(
        jnp.float32
    )
    list_sums = jnp.einsum(
        "rl,rm->lm", member, results.reshape(-1, subspaces), precision=lax.Precision.HIGHEST
    )
    counts = jnp.sum(member, axis=0)
    list_sums, counts = lax.psum((list_sums, counts), "gy")
    average = list_sums / jnp.maximum(counts, 1.0)[:, None]
    own_columns = subspaces // lax.axis_size("gy")
    list_error = lax.dynamic_slice_in_dim(
        average, lax.axis_index("gy") * own_columns, own_columns, 1
    )
    return (quant_error, list_error)


def solution(mesh):
    in_specs = (
        P(("gx", "gy"), None),
        P(("gx", "gy")),
        P(),
        P(),
        P("gx", "gy"),
        P(),
        P("gy", None, None),
    )
    out_specs = (P(("gx", "gy"), None), P("gx", "gy"))
    return jax.shard_map(
        on_device, mesh=mesh, in_specs=in_specs, out_specs=out_specs, check_vma=False
    )
```

```python
import functools

import jax
import jax.numpy as jnp
from jax import lax
from jax.experimental import pallas as pl
from jax.experimental.pallas import tpu as pltpu
from jax.sharding import PartitionSpec as P

LANES = 128
WIDE = 2 * LANES
F32 = jnp.float32
BF16 = jnp.bfloat16


VMEM = pl.BlockSpec(memory_space=pltpu.VMEM)


def on_chip(array):
    return pltpu.with_memory_space_constraint(array, pltpu.VMEM)


def iota_f32(shape, axis):
    return lax.broadcasted_iota(jnp.int32, shape, axis).astype(F32)


def dot(a, b, contract=((1,), (0,))):
    return lax.dot_general(a, b, (contract, ((), ())), preferred_element_type=F32)


def pick_lanes(rows, index):
    along = lax.GatherDimensionNumbers(
        offset_dims=(),
        collapsed_slice_dims=(1,),
        start_index_map=(1,),
        operand_batching_dims=(0,),
        start_indices_batching_dims=(0,),
    )
    return lax.gather(
        rows, index[..., None], along, slice_sizes=(1, 1), mode=lax.GatherScatterMode.PROMISE_IN_BOUNDS
    )


def slot_digits(ids_across, order_ref):
    order = order_ref[...].astype(jnp.int16)
    found = jnp.zeros((LANES, LANES), BF16)
    for block in range(order_ref.shape[0]):
        found = jnp.where(ids_across == order[block : block + 1, :], jnp.asarray(block + 1, BF16), found)
    found = found.astype(F32)
    hit = (found > 0.0).astype(F32)
    block_of = (found - hit).astype(BF16)
    ones = jnp.ones((8, LANES), BF16)
    lanes = iota_f32((8, LANES), 1).astype(BF16)
    slot = dot(ones, block_of, ((1,), (1,))) * float(LANES) + dot(lanes, hit.astype(BF16), ((1,), (1,)))
    high = jnp.floor(slot * (1.0 / WIDE))
    return high, slot - high * WIDE


def prepare_kernel(
    own, ids_hbm, old_hbm, new_hbm, vec_hbm, rot_hbm, cent_hbm, book_hbm,
    vec_ref, digit_ref, rot_ref, mine_ref, book_ref, ids_ref, old_ref, new_ref, arrived,
):
    side = lax.axis_index("gy")
    moves = (
        (ids_hbm, ids_ref),
        (old_hbm, old_ref),
        (new_hbm, new_ref),
        (rot_hbm, rot_ref),
        (vec_hbm, vec_ref),
        (cent_hbm.at[pl.ds(side * LANES, LANES)], mine_ref),
        (book_hbm.at[pl.ds(lax.axis_index("gx") * own, own)], book_ref),
    )
    copies = [pltpu.make_async_copy(src, dst, arrived.at[n]) for n, (src, dst) in enumerate(moves)]
    for copy in copies:
        copy.start()
    for copy in copies[:3]:
        copy.wait()
    ids_across = jnp.broadcast_to(ids_ref[...], (LANES, LANES)).astype(F32).T.astype(jnp.int32).astype(jnp.int16)
    old_high, old_low = slot_digits(ids_across, old_ref)
    new_high, new_low = slot_digits(ids_across, new_ref)
    row = lax.broadcasted_iota(jnp.int32, (8, LANES), 0)
    digits = jnp.where(row == 0, old_high, jnp.where(row == 1, old_low, jnp.where(row == 2, new_high, new_low)))
    digit_ref[...] = digits.astype(BF16)
    for copy in copies[3:]:
        copy.wait()


def code_table(words):
    own = len(words)
    row = lax.broadcasted_iota(jnp.int32, words[0].shape, 0)
    parts, tails = [], []
    for m, word in enumerate(words):
        zero = jnp.zeros_like(word)
        parts.append(jnp.concatenate([-2.0 * word if n == m else zero for n in range(own)], axis=1))
        norm = jnp.sum(word * word, axis=0, keepdims=True)
        top = norm.astype(BF16).astype(F32)
        middle = (norm - top).astype(BF16).astype(F32)
        low = norm - top - middle
        tails.append(jnp.where(row == 0, top, jnp.where(row == 1, middle, jnp.where(row == 2, low, 0.0))))
    parts.append(jnp.concatenate(tails, axis=1))
    return jnp.concatenate(parts, axis=0).T.astype(BF16)


def pack_kernel(mine_ref, other_ref, rot_ref, vec_ref, digit_ref, book_ref, out_ref, code_ref):
    side = lax.axis_index("gy")
    half = mine_ref.shape[1]
    own, sub_width = book_ref.shape[:2]
    width = own * sub_width
    rotated = jnp.zeros((2 * LANES, rot_ref.shape[1]), F32)
    for at, cents in ((side, mine_ref[...]), (1 - side, other_ref[pl.ds(side * LANES, LANES), :])):
        rows = jnp.concatenate([vec_ref[:, pl.ds(at * half, half)], cents], axis=0)
        rotated += dot(rows, rot_ref[pl.ds(at * half, half), :])
    code_ref[...] = code_table([book_ref[m].astype(F32) for m in range(own)])
    turned = rotated.T
    vectors, cents = turned[:, :LANES], turned[:, LANES:]
    digits = digit_ref[...].astype(F32)
    for device in range(out_ref.shape[0]):
        for part in range(width // 4):
            at = (device % 2) * half + (device // 2) * width + 4 * part
            out_ref[device, part] = vectors[at : at + 4].astype(BF16)
            out_ref[device, width // 4 + part] = cents[at : at + 4].astype(BF16)
        out_ref[device, width // 2] = digits[0:4].astype(BF16)


def encode_kernel(own, sub_width, in_ref, code_ref, out_ref, table_ref, low_ref):
    devices = in_ref.shape[0]
    tiles = devices // 2
    width = own * sub_width
    parts = width // 4
    codes = code_ref.shape[0] // own

    def stack(device, first):
        return jnp.concatenate([in_ref[device, first + n].astype(F32) for n in range(parts)], axis=0)

    digits = [in_ref[device, 2 * parts].astype(F32) for device in range(devices)]
    for tile in range(tiles):
        rows = jnp.concatenate([stack(2 * tile, parts), stack(2 * tile + 1, parts)], axis=0)
        table_ref[tile] = rows.astype(BF16)
    lane = lax.broadcasted_iota(jnp.int32, (WIDE, WIDE), 0).astype(F32)
    tail = (lax.broadcasted_iota(jnp.int32, (8, LANES), 0) < 3).astype(F32)
    code = code_ref[...]

    def turn(device):
        chunks = 2 * width // 16
        group = jnp.broadcast_to(digits[device][0:1], (16, LANES)).astype(BF16)
        place = digits[device][1:2]
        odd = place >= float(LANES)
        index = jnp.where(odd, place - float(LANES), place).astype(jnp.int32)
        index = jnp.broadcast_to(index, (16, LANES)).astype(jnp.int16)
        found = [jnp.zeros((16, LANES), BF16) for _ in range(chunks)]
        for tile in range(tiles):
            here = group == jnp.asarray(tile, BF16)
            for n in range(chunks):
                found[n] = jnp.where(here, pick_lanes(table_ref[tile, 16 * n : 16 * n + 16, :], index), found[n])
        both = jnp.concatenate([part.astype(F32) for part in found], axis=0)
        odd = jnp.broadcast_to(odd, (width, LANES))
        turned = stack(device, 0) - jnp.where(odd, both[width:], both[:width])
        low_ref[device] = jnp.concatenate([turned, tail], axis=0).astype(BF16)
        squared = turned * turned
        return jnp.concatenate(
            [jnp.sum(squared[8 * n : 8 * n + 8], axis=0, keepdims=True) for n in range(own)], axis=0
        )

    def measure(tile, squares):
        low = jnp.concatenate([low_ref[2 * tile], low_ref[2 * tile + 1]], axis=1)
        distance = dot(code, low)
        nearest = [jnp.min(distance[m * codes : (m + 1) * codes], axis=0, keepdims=True) for m in range(own)]
        return jnp.concatenate(nearest, axis=0) + jnp.concatenate(squares, axis=1)

    def gather(tile, error, sums):
        pair = jnp.concatenate([digits[2 * tile], digits[2 * tile + 1]], axis=1)
        for side in range(2):
            out_ref[2 * tile + side, 0] = error[0:2, side * LANES : (side + 1) * LANES].astype(BF16)
        rows = jnp.concatenate([error, jnp.ones((1, WIDE), F32)] * 2, axis=0)
        high = jnp.broadcast_to(pair[2:3], (8, WIDE)) - upper
        spread = jnp.concatenate(
            [jnp.where(high == float(group), rows, 0.0) for group in range(0, tiles, 2)], axis=0
        )
        hot = (pair[3:4] == lane).astype(F32).astype(BF16)
        return sums + dot(spread.astype(BF16), hot, ((1,), (1,)))

    upper = (lax.broadcasted_iota(jnp.int32, (8, WIDE), 0) >= 4).astype(F32)
    sums = jnp.zeros((tiles * 4, WIDE), F32)
    errors = []
    squares = [[turn(0), turn(1)]]
    for tile in range(tiles):
        if tile + 1 < tiles:
            squares.append([turn(2 * tile + 2), turn(2 * tile + 3)])
        errors.append(measure(tile, squares[tile]))
        if tile > 1:
            sums = gather(tile - 2, errors[tile - 2], sums)
    for tile in (tiles - 2, tiles - 1):
        sums = gather(tile, errors[tile], sums)
    spare = jnp.zeros((1, LANES), BF16)
    for tile in range(tiles):
        group = sums[tile * 4 : (tile + 1) * 4]
        mean = group[0:own] / jnp.maximum(group[own : own + 1], 1.0)
        left, right = mean[:, :LANES], mean[:, LANES:]
        last = jnp.concatenate([right[2:own].astype(BF16), spare], axis=0)
        for side in range(2):
            device = 2 * tile + side
            error = errors[tile][2:own, side * LANES : (side + 1) * LANES]
            out_ref[device, 1] = left[0:2].astype(BF16)
            out_ref[device, 2] = right[0:2].astype(BF16)
            out_ref[device, 3] = jnp.concatenate([error, left[2:own]], axis=0).astype(BF16)
            out_ref[device, 4] = last


def finish_kernel(own, in_ref, quant_ref, list_ref):
    tiles = in_ref.shape[0] // 2
    side = lax.axis_index("gy")
    for device in range(2 * tiles):
        at = ((device % 2) * tiles + device // 2) * own
        quant_ref[at : at + 2, :] = in_ref[device, 0].astype(F32)
        quant_ref[at + 2 : at + own, :] = in_ref[device, 3].astype(F32)[0:1]
    for tile in range(tiles):
        at, device = tile * own, 2 * tile + side
        list_ref[at : at + 2, 0:LANES] = in_ref[device, 1].astype(F32)
        list_ref[at : at + 2, LANES:WIDE] = in_ref[device, 2].astype(F32)
        list_ref[at + 2 : at + own, 0:LANES] = in_ref[device, 3].astype(F32)[1:2]
        list_ref[at + 2 : at + own, LANES:WIDE] = in_ref[device, 4].astype(F32)[0:1]


def on_device_by_column(vectors, list_ids, old_order, new_order, centroids, rotation, codebook):
    owners, sides = lax.axis_size("gx"), lax.axis_size("gy")
    devices = owners * sides
    subspaces, sub_width, codes = codebook.shape
    own = subspaces // owners
    width = own * sub_width
    features = vectors.shape[1]
    total = subspaces * sides
    other = lax.ppermute(centroids, "gy", [(0, 1), (1, 0)])
    vectors, digits, rotation, mine, book = pl.pallas_call(
        functools.partial(prepare_kernel, own),
        out_shape=(
            pltpu.VMEM((LANES, features), BF16),
            pltpu.VMEM((8, LANES), BF16),
            pltpu.VMEM(rotation.shape, BF16),
            pltpu.VMEM((LANES, centroids.shape[1]), BF16),
            pltpu.VMEM((own, sub_width, codes), BF16),
        ),
        in_specs=[pl.BlockSpec(memory_space=pl.ANY)] * 7,
        out_specs=(VMEM,) * 5,
        scratch_shapes=[
            pltpu.VMEM((1, LANES), jnp.int32),
            pltpu.VMEM((old_order.shape[0] // LANES, LANES), jnp.int32),
            pltpu.VMEM((old_order.shape[0] // LANES, LANES), jnp.int32),
            pltpu.SemaphoreType.DMA((7,)),
        ],
        name="prepare",
    )(
        list_ids.reshape(1, LANES),
        old_order.reshape(-1, LANES),
        new_order.reshape(-1, LANES),
        vectors,
        rotation,
        centroids,
        codebook,
    )
    outgoing, code = pl.pallas_call(
        pack_kernel,
        out_shape=(
            pltpu.VMEM((devices, width // 2 + 1, 4, LANES), BF16),
            pltpu.VMEM((own * codes, width + 8), BF16),
        ),
        in_specs=[VMEM] * 6,
        out_specs=(VMEM, VMEM),
        name="pack",
    )(*(on_chip(array) for array in (mine, other, rotation, vectors, digits, book)))
    incoming = lax.all_to_all(outgoing, ("gx", "gy"), split_axis=0, concat_axis=0, tiled=True)
    returning = pl.pallas_call(
        functools.partial(encode_kernel, own, sub_width),
        out_shape=pltpu.VMEM((devices, 5, 2, LANES), BF16),
        scratch_shapes=[
            pltpu.VMEM((owners, 2 * width, LANES), BF16),
            pltpu.VMEM((devices, width + 8, LANES), BF16),
        ],
        in_specs=[VMEM] * 2,
        out_specs=VMEM,
        name="encode",
    )(on_chip(incoming), on_chip(code))
    returned = lax.all_to_all(returning, ("gx", "gy"), split_axis=0, concat_axis=0, tiled=True)
    quant_error, list_error = pl.pallas_call(
        functools.partial(finish_kernel, own),
        out_shape=(
            jax.ShapeDtypeStruct((total, LANES), F32),
            jax.ShapeDtypeStruct((subspaces, WIDE), F32),
        ),
        in_specs=[VMEM],
        out_specs=(VMEM, VMEM),
        name="finish",
    )(on_chip(returned))
    return quant_error.T, list_error.T


def on_device(vectors, list_ids, old_order, new_order, centroids, rotation, codebook):
    owners, sides = lax.axis_size("gx"), lax.axis_size("gy")
    subspaces, sub_width, codes = codebook.shape
    own = subspaces // owners
    by_column = (
        sides == 2
        and own * owners == subspaces
        and own == 3
        and sub_width == 8
        and codes % LANES == 0
        and vectors.shape[0] == LANES
        and centroids.shape[0] == WIDE
        and old_order.shape[0] == owners * WIDE
        and owners <= LANES
        and owners % 2 == 0
    )
    plan = on_device_by_column if by_column else on_device_by_owner
    return plan(vectors, list_ids, old_order, new_order, centroids, rotation, codebook)


def subspace_errors(turned, codewords, code_norm):
    row_count = turned.shape[0]
    subspaces, sub_width, code_count = codewords.shape
    group_size = 8
    group_count = subspaces // group_size
    lowered = turned.astype(jnp.bfloat16).reshape(row_count, group_count, group_size, sub_width)
    lowered = jnp.moveaxis(lowered, 1, 0)
    squares = jnp.sum(
        (turned * turned).reshape(row_count, group_count, group_size, sub_width), axis=3
    )
    squares = jnp.moveaxis(squares, 1, 0)
    book_groups = codewords.reshape(group_count, group_size, sub_width, code_count)
    norm_groups = code_norm.reshape(group_count, group_size, code_count)

    def one_group(operands):
        lowered_part, square_part, book_part, norm_part = operands
        inner_terms = jnp.einsum(
            "rgd,gdk->rgk", lowered_part, book_part, preferred_element_type=jnp.float32
        )
        inner_terms = lax.optimization_barrier(inner_terms.astype(jnp.bfloat16)).astype(jnp.float32)
        distance = square_part[:, :, None] - 2.0 * inner_terms + norm_part[None, :, :]
        return jnp.min(distance, axis=2)

    nearest = lax.map(one_group, (lowered, squares, book_groups, norm_groups))
    return jnp.moveaxis(nearest, 0, 1).reshape(row_count, subspaces)


def on_device_by_owner(vectors, list_ids, old_order, new_order, centroids, rotation, codebook):
    owners = lax.axis_size("gx")
    owner_index = lax.axis_index("gx")
    lists_own = centroids.shape[0]
    list_total = old_order.shape[0]
    rows_dev = vectors.shape[0]
    feature_width = vectors.shape[1]
    capacity = 5 * rows_dev // (2 * owners)
    own_lists = lax.dynamic_slice_in_dim(new_order, owner_index * lists_own, lists_own)
    select = (own_lists[:, None] == old_order[None, :]).astype(jnp.bfloat16)
    own_part = jnp.dot(
        select,
        lax.all_gather(centroids, "gx", axis=0, tiled=True),
        preferred_element_type=jnp.float32,
    )
    own_centroids = lax.all_gather(own_part.astype(jnp.bfloat16), "gy", axis=1, tiled=True)
    rot_cent = jnp.dot(own_centroids, rotation, preferred_element_type=jnp.float32)
    padded_cent = jnp.concatenate([rot_cent, jnp.zeros((1, feature_width), jnp.float32)], axis=0)
    codewords = lax.all_gather(codebook, "gy", axis=0, tiled=True)
    code_float = codewords.astype(jnp.float32)
    code_norm = jnp.sum(code_float * code_float, axis=1)
    subspaces = codewords.shape[0]
    slot_of = (
        jnp.zeros((list_total,), jnp.int32)
        .at[new_order]
        .set(jnp.arange(list_total, dtype=jnp.int32))
    )
    new_slot = slot_of[list_ids]
    dest_owner = new_slot // lists_own
    local_list = new_slot % lists_own
    owner_hits = (dest_owner[:, None] == jnp.arange(owners, dtype=jnp.int32)[None, :]).astype(
        jnp.int32
    )
    before = jnp.cumsum(owner_hits, axis=0) - owner_hits
    position = jnp.sum(before * owner_hits, axis=1)
    target = dest_owner * capacity + position
    labels_flat = jnp.full((owners * capacity,), lists_own, jnp.int32).at[target].set(local_list)
    outgoing = jnp.zeros((owners * capacity, feature_width), jnp.bfloat16).at[target].set(vectors)
    incoming = lax.all_to_all(
        outgoing.reshape(owners, capacity, feature_width),
        "gx",
        split_axis=0,
        concat_axis=0,
        tiled=True,
    )
    labels = lax.all_to_all(
        labels_flat.astype(jnp.bfloat16).reshape(owners, capacity),
        "gx",
        split_axis=0,
        concat_axis=0,
        tiled=True,
    )
    turned = jnp.dot(
        incoming.reshape(-1, feature_width), rotation, preferred_element_type=jnp.float32
    )
    finish_turned = turned
    label_rows = labels.reshape(-1).astype(jnp.int32)
    finish_turned = finish_turned - jnp.take(padded_cent, label_rows, axis=0)
    errors = subspace_errors(finish_turned, codewords, code_norm)
    results = errors.reshape(labels.shape[0], labels.shape[1], subspaces)
    returned = lax.all_to_all(results, "gx", split_axis=0, concat_axis=0, tiled=True)
    quant_error = returned.reshape(owners * capacity, subspaces)[target]
    label_rows = labels.reshape(-1).astype(jnp.int32)
    member = (label_rows[:, None] == jnp.arange(lists_own, dtype=jnp.int32)[None, :]).astype(
        jnp.float32
    )
    list_sums = jnp.einsum(
        "rl,rm->lm", member, results.reshape(-1, subspaces), precision=lax.Precision.HIGHEST
    )
    counts = jnp.sum(member, axis=0)
    list_sums, counts = lax.psum((list_sums, counts), "gy")
    average = list_sums / jnp.maximum(counts, 1.0)[:, None]
    own_columns = subspaces // lax.axis_size("gy")
    list_error = lax.dynamic_slice_in_dim(
        average, lax.axis_index("gy") * own_columns, own_columns, 1
    )
    return (quant_error, list_error)


def solution(mesh):
    in_specs = (
        P(("gx", "gy"), None),
        P(("gx", "gy")),
        P(),
        P(),
        P("gx", "gy"),
        P(),
        P("gy", None, None),
    )
    out_specs = (P(("gx", "gy"), None), P("gx", "gy"))
    return jax.shard_map(
        on_device, mesh=mesh, in_specs=in_specs, out_specs=out_specs, check_vma=False
    )
```
